32 devices in a mesh: ens: 1 (over z), col: 4 (over y), row: 8 (over x, core).
Axes of the slice: x: 4, y: 4, z: 1, core: 2. Of those that a mesh axis runs over, the one named last changes fastest.
The devices are a block of a 4x4x8 slice.
Arguments:
- u_init: float32 [2048, 2048], P(('ens', 'row'), 'col')
- v_init: float32 [2048, 2048], P(('ens', 'row'), 'col')
- stencil_w: float32 [64, 3, 3], replicated
Outputs:
- output 1: float32 [2048, 2048], P(('ens', 'row'), 'col')
- output 2: float32 [2048, 2048], P(('ens', 'row'), 'col')
All inputs are finite; a program needn't handle non-finite values.
Results may differ from the reference program's by a relative error of at most 0.001.
Values are sent between devices in bfloat16 or wider.
A program may use at most 768 MiB of HBM per device.

```python
import jax
import jax.numpy as jnp
from jax import lax

GRID_ROWS = 2048
GRID_COLS = 2048
NUM_STEPS = 64
TIME_STEP = 0.5


def block_field(base_key, block_rows, block_cols):
    block_vals = jax.random.normal(base_key, (GRID_ROWS // block_rows, GRID_COLS // block_cols), jnp.float32)
    spread = jnp.broadcast_to(block_vals[:, None, :, None], (GRID_ROWS // block_rows, block_rows, GRID_COLS // block_cols, block_cols))
    return spread.reshape(GRID_ROWS, GRID_COLS)


def setup_inputs(seed: int = 0, part: int = 0) -> dict:
    part_key = jax.random.fold_in(jax.random.key(seed), part)
    key_ublock, key_unoise, key_vblock, key_vnoise = jax.random.split(part_key, 4)
    u_init = block_field(key_ublock, 8, 8) + 0.3 * jax.random.normal(key_unoise, (GRID_ROWS, GRID_COLS), jnp.float32)
    v_init = 0.5 * block_field(key_vblock, 8, 8) + 0.2 * jax.random.normal(key_vnoise, (GRID_ROWS, GRID_COLS), jnp.float32)
    key_pair, key_centre, key_total = jax.random.split(jax.random.key(seed + 1), 3)
    pair_weights = jax.random.uniform(key_pair, (NUM_STEPS, 4), jnp.float32, minval=0.07, maxval=0.13)
    centre = jax.random.uniform(key_centre, (NUM_STEPS,), jnp.float32, minval=0.2, maxval=0.35)
    weight_total = jax.random.uniform(key_total, (NUM_STEPS,), jnp.float32, minval=0.93, maxval=0.98)
    raw_weights = jnp.stack([
        pair_weights[:, 2], pair_weights[:, 0], pair_weights[:, 3],
        pair_weights[:, 1], centre, pair_weights[:, 1],
        pair_weights[:, 3], pair_weights[:, 0], pair_weights[:, 2]], axis=1)
    weight_scale = weight_total / jnp.sum(raw_weights, axis=1)
    stencil_w = (raw_weights * weight_scale[:, None]).reshape(NUM_STEPS, 3, 3)
    return {"u_init": u_init, "v_init": v_init, "stencil_w": stencil_w}


def stencil_sum(field_now, step_w):
    total_acc = step_w[0, 0] * jnp.roll(field_now, (1, 1), axis=(0, 1))
    for tap_index in range(1, 9):
        row_off, col_off = divmod(tap_index, 3)
        total_acc = total_acc + step_w[row_off, col_off] * jnp.roll(field_now, (1 - row_off, 1 - col_off), axis=(0, 1))
    return total_acc


def reference(u_init, v_init, stencil_w):
    def one_step(state_pair, step_w):
        u_now, v_now = state_pair
        v_next = v_now + (stencil_sum(u_now, step_w) - u_now)
        u_next = u_now + TIME_STEP * v_next
        return (u_next, v_next), None

    (u_final, v_final), _ = lax.scan(one_step, (u_init, v_init), stencil_w)
    return (u_final, v_final)
```

```python
import functools

import jax
import jax.numpy as jnp
from jax import lax
from jax.experimental import pallas as pl
from jax.experimental.pallas import tpu as pltpu
from jax.sharding import PartitionSpec as P

LANES = 128
SUB = 8
NC = 5
MESH = pl.DeviceIdType.MESH


def lane_iota():
    return lax.broadcasted_iota(jnp.int32, (SUB, LANES), 1)


def permute(x, idx):
    return jnp.take_along_axis(x, idx, axis=1, mode="promise_in_bounds")


def pick(masks, parts):
    out = parts[0]
    for m, p in zip(masks[1:], parts[1:]):
        out = jnp.where(m, p, out)
    return out


def step_coeffs(w_ref, t):
    w = [[jnp.full((SUB, LANES), w_ref[a, b, t]) for b in range(3)] for a in range(2)]
    return (
        0.5 * w[0][1],
        0.5 * w[1][0],
        0.25 * (w[0][0] + w[0][2]),
        0.25 * (w[0][0] - w[0][2]),
        1.5 + 0.5 * w[1][1],
    )


def stencil_group(cur, prv, coeffs, r0):
    w01, w10, al, be, cc = coeffs
    above = cur[:, pl.ds(r0 - 1, SUB), :]
    mid = cur[:, pl.ds(r0, SUB), :]
    below = cur[:, pl.ds(r0 + 1, SUB), :]
    s = above + below
    q = al * s + w10 * mid
    r = be * (above - below)
    x = q + r
    y = q - r
    z = (w01 * s + cc * mid) - prv[:, pl.ds(r0, SUB), :]
    x_wrap = pltpu.roll(x[NC - 1], 1, 1)
    y_wrap = pltpu.roll(y[0], LANES - 1, 1)
    for c in range(NC):
        xc = x[c - 1] if c else x_wrap
        yc = y[c + 1] if c < NC - 1 else y_wrap
        prv[c, pl.ds(r0, SUB), :] = (z[c] + xc) + yc


def exchange(
    rows, cols, kr, halo, row_n, col_n,
    u_ref, v_ref, ru, rv, h_l, h_r,
    edge, pk_l, pk_r, in_sem, send_sem, recv_sem,
):
    my_row, my_col = lax.axis_index("row"), lax.axis_index("col")
    up, down = lax.rem(my_row + row_n - 1, row_n), lax.rem(my_row + 1, row_n)
    left, right = lax.rem(my_col + col_n - 1, col_n), lax.rem(my_col + 1, col_n)
    loads = []
    for i, (ref, col) in enumerate(((u_ref, 0), (v_ref, 0), (u_ref, cols - LANES), (v_ref, cols - LANES))):
        loads.append(pltpu.make_async_copy(ref.at[:, pl.ds(col, LANES)], edge.at[i], in_sem.at[i]))
        loads[-1].start()
    barrier = pltpu.get_barrier_semaphore()
    around = [(r, c) for r in (up, my_row, down) for c in (left, my_col, right)]
    around = [d for i, d in enumerate(around) if i != 4]
    for r, c in around:
        pl.semaphore_signal(barrier, inc=1, device_id={"row": r, "col": c}, device_id_type=MESH)
    for c in loads:
        c.wait()
    low = lane_iota() < halo

    def pack(g, _):
        at = pl.ds(pl.multiple_of(SUB * g, SUB), SUB)
        pk_l[at, :] = jnp.where(low, edge[0, at, :], pltpu.roll(edge[1, at, :], halo, 1))
        pk_r[at, :] = jnp.where(low, pltpu.roll(edge[3, at, :], halo, 1), edge[2, at, :])
        return 0

    lax.fori_loop(0, rows // SUB, pack, 0, unroll=8)
    pl.semaphore_wait(barrier, len(around))
    sends = []

    def send(src, dst, r, c):
        i = len(sends)
        copy = pltpu.make_async_remote_copy(
            src_ref=src, dst_ref=dst, send_sem=send_sem.at[i], recv_sem=recv_sem.at[i],
            device_id={"row": r, "col": c}, device_id_type=MESH,
        )
        copy.start()
        sends.append(copy)

    own, top, bottom = pl.ds(kr, rows), pl.ds(0, kr), pl.ds(kr + rows, kr)
    send(pk_l, h_r.at[own], my_row, left)
    send(pk_r, h_l.at[own], my_row, right)
    for n, r in ((u_ref, ru), (v_ref, rv)):
        send(n.at[pl.ds(0, kr)], r.at[pl.ds(kr, kr)], up, my_col)
        send(n.at[pl.ds(rows - kr, kr)], r.at[pl.ds(0, kr)], down, my_col)
    send(pk_l.at[pl.ds(0, kr)], h_r.at[bottom], up, left)
    send(pk_l.at[pl.ds(rows - kr, kr)], h_r.at[top], down, left)
    send(pk_r.at[pl.ds(0, kr)], h_l.at[bottom], up, right)
    send(pk_r.at[pl.ds(rows - kr, kr)], h_l.at[top], down, right)
    for c in sends:
        c.wait()


def kernel(
    rows, cols, steps, kr, halo,
    u_ref, v_ref, w_ref, ru, rv, h_l, h_r, uo_ref, vo_ref,
    nu, nv, x0, x1, in_sem, out_sem,
):
    own = pl.ds(0, rows)
    loads = [
        pltpu.make_async_copy(u_ref, nu, in_sem.at[0]),
        pltpu.make_async_copy(v_ref, nv, in_sem.at[1]),
    ]
    for c in loads:
        c.start()
    for c in loads:
        c.wait()
    lane = lane_iota()
    low = lane < halo
    nblk = cols // LANES

    residue = lax.rem(lane, NC)
    masks = [residue == m for m in range(NC)]

    def to_lanes(nu, nv, at, row0):
        out_row = SUB + row0
        hl, hr = h_l[pl.ds(row0, SUB), :], h_r[pl.ds(row0, SUB), :]
        uh = jnp.where(low, hr, hl)
        vh = pltpu.roll(jnp.where(low, hl, hr), halo, 1)
        ub = [nu[at, b * LANES : (b + 1) * LANES] for b in range(nblk)] + [uh]
        vb = [nv[at, b * LANES : (b + 1) * LANES] for b in range(nblk)] + [vh]
        for c in range(NC):
            idx = (NC * lane + (c - halo) % LANES) & (LANES - 1)
            res = [(c - halo - LANES * b) % NC for b in range(nblk + 1)]
            sel = [masks[k] for k in res]
            ul = 0.25 * permute(pick(sel, ub), idx)
            vl = permute(pick(sel, vb), idx)
            x0[c, pl.ds(out_row, SUB), :] = ul
            x1[c, pl.ds(out_row, SUB), :] = ul - 0.125 * vl

    for g in range(kr // SUB):
        to_lanes(ru, rv, pl.ds(SUB * g, SUB), SUB * g)
    for g in range(rows // SUB):
        to_lanes(nu, nv, pl.ds(SUB * g, SUB), kr + SUB * g)
    for g in range(kr // SUB):
        to_lanes(ru, rv, pl.ds(kr + SUB * g, SUB), kr + rows + SUB * g)

    base = SUB + kr
    done = 0
    while done < steps:
        left_steps = steps - done
        count = min(SUB, left_steps)
        ext = -(-(left_steps - 1) // SUB) * SUB

        def two(i, _, done=done, ext=ext):
            for j, (a, b) in enumerate(((x0, x1), (x1, x0))):
                coeffs = step_coeffs(w_ref, done + 2 * i + j)
                for r0 in range(base - ext, base + rows + ext, SUB):
                    stencil_group(a, b, coeffs, r0)
            return 0

        lax.fori_loop(0, count // 2, two, 0)
        done += count

    inv = pow(NC, -1, LANES)
    for g in range(rows // SUB):
        at = pl.ds(base + SUB * g, SUB)
        to = pl.ds(SUB * g, SUB)
        uu, vv = [], []
        for c in range(NC):
            idx = (inv * (lane + (halo - c) % LANES)) & (LANES - 1)
            now, old = x0[c, at, :], x1[c, at, :]
            uu.append(permute(4.0 * now, idx))
            vv.append(permute(8.0 * (now - old), idx))
        for b in range(nblk):
            sel = [masks[(c - halo - LANES * b) % NC] for c in range(NC)]
            nu[to, b * LANES : (b + 1) * LANES] = pick(sel, uu)
            nv[to, b * LANES : (b + 1) * LANES] = pick(sel, vv)
    stores = [
        pltpu.make_async_copy(nu.at[own], uo_ref, out_sem.at[0]),
        pltpu.make_async_copy(nv.at[own], vo_ref, out_sem.at[1]),
    ]
    for c in stores:
        c.start()
    for c in stores:
        c.wait()


def solution(mesh):
    row_n, col_n = mesh.shape["row"], mesh.shape["col"]
    spec = P(("ens", "row"), "col")

    def local_run(u, v, w):
        rows, cols = u.shape
        steps = w.shape[0]
        kr = -(-steps // SUB) * SUB
        halo = (NC * LANES - cols) // 2
        tall = rows + 2 * kr
        f32 = jnp.float32
        any_space = pl.BlockSpec(memory_space=pl.ANY)
        vmem = pl.BlockSpec(memory_space=pltpu.VMEM)
        smem = pl.BlockSpec(memory_space=pltpu.SMEM)
        halos = pl.pallas_call(
            functools.partial(exchange, rows, cols, kr, halo, row_n, col_n),
            out_shape=[jax.ShapeDtypeStruct((2 * kr, cols), f32)] * 2
            + [jax.ShapeDtypeStruct((tall, LANES), f32)] * 2,
            in_specs=[any_space] * 2,
            out_specs=[vmem] * 4,
            scratch_shapes=[
                pltpu.VMEM((4, rows, LANES), f32),
                pltpu.VMEM((rows, LANES), f32),
                pltpu.VMEM((rows, LANES), f32),
                pltpu.SemaphoreType.DMA((4,)),
                pltpu.SemaphoreType.DMA((10,)),
                pltpu.SemaphoreType.DMA((10,)),
            ],
            compiler_params=pltpu.CompilerParams(collective_id=0, has_side_effects=True),
        )(u, v)
        out = jax.ShapeDtypeStruct(u.shape, f32)
        return pl.pallas_call(
            functools.partial(kernel, rows, cols, steps, kr, halo),
            out_shape=(out, out),
            in_specs=[any_space, any_space, smem] + [vmem] * 4,
            out_specs=(any_space, any_space),
            scratch_shapes=[
                pltpu.VMEM((rows, cols), f32),
                pltpu.VMEM((rows, cols), f32),
                pltpu.VMEM((NC, tall + 2 * SUB, LANES), f32),
                pltpu.VMEM((NC, tall + 2 * SUB, LANES), f32),
                pltpu.SemaphoreType.DMA((2,)),
                pltpu.SemaphoreType.DMA((2,)),
            ],
        )(u, v, jnp.transpose(w, (1, 2, 0)), *halos)

    return jax.shard_map(
        local_run, mesh=mesh, in_specs=(spec, spec, P()), out_specs=(spec, spec), check_vma=False
    )
```

```python
import functools

import jax
import jax.numpy as jnp
from jax import lax
from jax.experimental import pallas as pl
from jax.experimental.pallas import tpu as pltpu
from jax.sharding import PartitionSpec as P

LANES = 128
SUB = 8
NC = 5
PAD = 3 * SUB
MESH = pl.DeviceIdType.MESH


def lane_iota():
    return lax.broadcasted_iota(jnp.int32, (SUB, LANES), 1)


def permute(x, idx):
    return jnp.take_along_axis(x, idx, axis=1, mode="promise_in_bounds")


def pick(masks, parts):
    out = parts[0]
    for m, p in zip(masks[1:], parts[1:]):
        out = jnp.where(m, p, out)
    return out


def step_coeffs(w_ref, t):
    w = [[jnp.full((SUB, LANES), w_ref[a, b, t]) for b in range(3)] for a in range(2)]
    return (
        0.5 * w[0][1],
        0.5 * w[1][0],
        0.25 * (w[0][0] + w[0][2]),
        0.25 * (w[0][0] - w[0][2]),
        1.5 + 0.5 * w[1][1],
    )


def stencil_group(cur, prv, coeffs, r0):
    w01, w10, al, be, cc = coeffs
    above = cur[:, pl.ds(r0 - 1, SUB), :]
    mid = cur[:, pl.ds(r0, SUB), :]
    below = cur[:, pl.ds(r0 + 1, SUB), :]
    s = above + below
    q = al * s + w10 * mid
    r = be * (above - below)
    x = q + r
    y = q - r
    z = (w01 * s + cc * mid) - prv[:, pl.ds(r0, SUB), :]
    x_wrap = pltpu.roll(x[NC - 1], 1, 1)
    y_wrap = pltpu.roll(y[0], LANES - 1, 1)
    for c in range(NC):
        xc = x[c - 1] if c else x_wrap
        yc = y[c + 1] if c < NC - 1 else y_wrap
        prv[c, pl.ds(r0, SUB), :] = (z[c] + xc) + yc


def kernel(
    rows, cols, steps, kr, halo, row_n, col_n,
    u_ref, v_ref, w_ref, uo_ref, vo_ref,
    nu, nv, pk_l, pk_r, h_l, h_r, x0, x1, got,
    in_sem, out_sem, send_sem, recv_sem, edge_send, edge_recv,
):
    my_row, my_col = lax.axis_index("row"), lax.axis_index("col")
    up, down = lax.rem(my_row + row_n - 1, row_n), lax.rem(my_row + 1, row_n)
    left, right = lax.rem(my_col + col_n - 1, col_n), lax.rem(my_col + 1, col_n)
    own = pl.ds(kr, rows)
    loads = [
        pltpu.make_async_copy(u_ref, nu.at[own], in_sem.at[0]),
        pltpu.make_async_copy(v_ref, nv.at[own], in_sem.at[1]),
    ]
    for c in loads:
        c.start()
    barrier = pltpu.get_barrier_semaphore()
    around = [(r, c) for r in (up, my_row, down) for c in (left, my_col, right)]
    around = [d for i, d in enumerate(around) if i != 4]
    for r, c in around:
        pl.semaphore_signal(barrier, inc=1, device_id={"row": r, "col": c}, device_id_type=MESH)
    for c in loads:
        c.wait()
    lane = lane_iota()
    low = lane < halo
    nblk = cols // LANES

    def pack(g, _):
        src = pl.ds(pl.multiple_of(kr + SUB * g, SUB), SUB)
        dst = pl.ds(pl.multiple_of(SUB * g, SUB), SUB)
        u_first, v_first = nu[src, :LANES], nv[src, :LANES]
        u_last, v_last = nu[src, cols - LANES :], nv[src, cols - LANES :]
        pk_l[dst, :] = jnp.where(low, u_first, pltpu.roll(v_first, halo, 1))
        pk_r[dst, :] = jnp.where(low, pltpu.roll(v_last, halo, 1), u_last)
        return 0

    lax.fori_loop(0, rows // SUB, pack, 0, unroll=8)
    pl.semaphore_wait(barrier, len(around))
    sends = []

    def send(src, dst, r, c):
        i = len(sends)
        copy = pltpu.make_async_remote_copy(
            src_ref=src, dst_ref=dst, send_sem=send_sem.at[i], recv_sem=recv_sem.at[i],
            device_id={"row": r, "col": c}, device_id_type=MESH,
        )
        copy.start()
        sends.append(copy)

    top, bottom = pl.ds(0, kr), pl.ds(kr + rows, kr)
    send(pk_l, h_r.at[own], my_row, left)
    send(pk_r, h_l.at[own], my_row, right)
    for n in (nu, nv):
        send(n.at[pl.ds(kr, kr)], n.at[bottom], up, my_col)
        send(n.at[pl.ds(rows, kr)], n.at[top], down, my_col)
    send(pk_l.at[pl.ds(0, kr)], h_r.at[bottom], up, left)
    send(pk_l.at[pl.ds(rows - kr, kr)], h_r.at[top], down, left)
    send(pk_r.at[pl.ds(0, kr)], h_l.at[bottom], up, right)
    send(pk_r.at[pl.ds(rows - kr, kr)], h_l.at[top], down, right)
    for c in sends:
        c.wait()

    residue = lax.rem(lane, NC)
    masks = [residue == m for m in range(NC)]
    base = PAD

    def to_lanes(g, _):
        at = pl.ds(pl.multiple_of(SUB * g, SUB), SUB)
        out = pl.ds(pl.multiple_of(base - kr + SUB * g, SUB), SUB)
        hl, hr = h_l[at, :], h_r[at, :]
        uh = jnp.where(low, hr, hl)
        vh = pltpu.roll(jnp.where(low, hl, hr), halo, 1)
        ub = [nu[at, b * LANES : (b + 1) * LANES] for b in range(nblk)] + [uh]
        vb = [nv[at, b * LANES : (b + 1) * LANES] for b in range(nblk)] + [vh]
        for c in range(NC):
            idx = (NC * lane + (c - halo) % LANES) & (LANES - 1)
            sel = [masks[(c - halo - LANES * b) % NC] for b in range(nblk + 1)]
            ul = 0.25 * permute(pick(sel, ub), idx)
            vl = permute(pick(sel, vb), idx)
            x0[c, out, :] = ul
            x1[c, out, :] = ul - 0.125 * vl
        return 0

    lax.fori_loop(0, (rows + 2 * kr) // SUB, to_lanes, 0, unroll=4)

    par = lax.rem(my_row, 2)
    sign = 2 * par - 1
    cut = rows // 2
    n_big = (cut + kr) // SUB
    partners = (lax.rem(my_row + sign + row_n, row_n), lax.rem(my_row - sign + row_n, row_n))
    edge_at = ((rows - kr) * par, (rows - kr) * (1 - par))
    halo_at = ((rows + kr) * par - kr, rows - (rows + kr) * par)

    def edge_copies(half, p):
        slot = lax.rem(p, 2)
        src = pl.ds(pl.multiple_of(base + edge_at[half], SUB), kr)
        return [
            pltpu.make_async_remote_copy(
                src_ref=x.at[:, src, :], dst_ref=got.at[half, slot, i],
                send_sem=edge_send.at[half, slot, i], recv_sem=edge_recv.at[half, slot, i],
                device_id={"row": partners[half]}, device_id_type=MESH,
            )
            for i, x in enumerate((x0, x1))
        ]

    def half_steps(half, t_base, t0, count, n):
        start = (cut - SUB * n * (1 - par), cut - SUB * n * par)[half]

        def two(i, _):
            for j, (a, b) in enumerate(((x0, x1), (x1, x0))):
                t = t0 + 2 * i + j
                coeffs = step_coeffs(w_ref, t_base + t)
                r0 = base + start + sign * t
                for g in range(n):
                    stencil_group(a, b, coeffs, r0 + SUB * g)
            return 0

        lax.fori_loop(0, count // 2, two, 0)

    n_phase = steps // kr

    def phase(p, _):
        for half in range(2):
            @pl.when(p > 0)
            def _():
                for c in edge_copies(half, p - 1):
                    c.wait()
                slot = lax.rem(p - 1, 2)
                dst = pl.ds(pl.multiple_of(base + halo_at[half], SUB), kr)
                x0[:, dst, :] = got[half, slot, 0]
                x1[:, dst, :] = got[half, slot, 1]

            n_late = n_big - kr // SUB if half == 0 else n_big
            half_steps(half, kr * p, 0, kr // 2, n_big)
            half_steps(half, kr * p, kr // 2, kr // 2, n_late)

            @pl.when(p < n_phase - 1)
            def _():
                for c in edge_copies(half, p):
                    c.start()
        return 0

    lax.fori_loop(0, n_phase, phase, 0)

    inv = pow(NC, -1, LANES)

    def to_natural(g, _):
        at = pl.ds(pl.multiple_of(base + SUB * g, SUB), SUB)
        to = pl.ds(pl.multiple_of(kr + SUB * g, SUB), SUB)
        uu, vv = [], []
        for c in range(NC):
            idx = (inv * (lane + (halo - c) % LANES)) & (LANES - 1)
            now, old = x0[c, at, :], x1[c, at, :]
            uu.append(permute(4.0 * now, idx))
            vv.append(permute(8.0 * (now - old), idx))
        for b in range(nblk):
            sel = [masks[(c - halo - LANES * b) % NC] for c in range(NC)]
            nu[to, b * LANES : (b + 1) * LANES] = pick(sel, uu)
            nv[to, b * LANES : (b + 1) * LANES] = pick(sel, vv)
        return 0

    lax.fori_loop(0, rows // SUB, to_natural, 0, unroll=4)
    stores = [
        pltpu.make_async_copy(nu.at[own], uo_ref, out_sem.at[0]),
        pltpu.make_async_copy(nv.at[own], vo_ref, out_sem.at[1]),
    ]
    for c in stores:
        c.start()
    for c in stores:
        c.wait()


def solution(mesh):
    row_n, col_n = mesh.shape["row"], mesh.shape["col"]
    spec = P(("ens", "row"), "col")

    def local_run(u, v, w):
        rows, cols = u.shape
        steps = w.shape[0]
        kr = 2 * SUB
        halo = (NC * LANES - cols) // 2
        tall = rows + 2 * kr
        f32 = jnp.float32
        out = jax.ShapeDtypeStruct(u.shape, f32)
        return pl.pallas_call(
            functools.partial(kernel, rows, cols, steps, kr, halo, row_n, col_n),
            out_shape=(out, out),
            in_specs=[
                pl.BlockSpec(memory_space=pl.ANY),
                pl.BlockSpec(memory_space=pl.ANY),
                pl.BlockSpec(memory_space=pltpu.SMEM),
            ],
            out_specs=(pl.BlockSpec(memory_space=pl.ANY), pl.BlockSpec(memory_space=pl.ANY)),
            scratch_shapes=[
                pltpu.VMEM((tall, cols), f32),
                pltpu.VMEM((tall, cols), f32),
                pltpu.VMEM((rows, LANES), f32),
                pltpu.VMEM((rows, LANES), f32),
                pltpu.VMEM((tall, LANES), f32),
                pltpu.VMEM((tall, LANES), f32),
                pltpu.VMEM((NC, rows + 2 * PAD, LANES), f32),
                pltpu.VMEM((NC, rows + 2 * PAD, LANES), f32),
                pltpu.VMEM((2, 2, 2, NC, kr, LANES), f32),
                pltpu.SemaphoreType.DMA((2,)),
                pltpu.SemaphoreType.DMA((2,)),
                pltpu.SemaphoreType.DMA((10,)),
                pltpu.SemaphoreType.DMA((10,)),
                pltpu.SemaphoreType.DMA((2, 2, 2)),
                pltpu.SemaphoreType.DMA((2, 2, 2)),
            ],
            compiler_params=pltpu.CompilerParams(collective_id=0, has_side_effects=True),
        )(u, v, jnp.transpose(w, (1, 2, 0)))

    return jax.shard_map(
        local_run, mesh=mesh, in_specs=(spec, spec, P()), out_specs=(spec, spec), check_vma=False
    )
```

```python
import functools

import jax
import jax.numpy as jnp
from jax import lax
from jax.experimental import pallas as pl
from jax.experimental.pallas import tpu as pltpu
from jax.sharding import PartitionSpec as P

LANES = 128
SUB = 8
NC = 5
UNROLL = 4
FIRST = 10
PAD = 3 * SUB
MESH = pl.DeviceIdType.MESH


def lane_iota():
    return lax.broadcasted_iota(jnp.int32, (SUB, LANES), 1)


def permute(x, idx):
    return lax.gather(
        x, idx[..., None],
        lax.GatherDimensionNumbers(
            offset_dims=(), collapsed_slice_dims=(1,), start_index_map=(1,),
            operand_batching_dims=(0,), start_indices_batching_dims=(0,),
        ),
        slice_sizes=(1, 1), mode=lax.GatherScatterMode.PROMISE_IN_BOUNDS,
    )


def pick(masks, parts):
    out = parts[0]
    for m, p in zip(masks[1:], parts[1:]):
        out = jnp.where(m, p, out)
    return out


def step_coeffs(w_ref, t):
    w = [[jnp.full((SUB, LANES), w_ref[a, b, t]) for b in range(3)] for a in range(2)]
    return (
        0.5 * w[0][1],
        0.5 * w[1][0],
        0.25 * (w[0][0] + w[0][2]),
        0.25 * (w[0][0] - w[0][2]),
        1.5 + 0.5 * w[1][1],
    )


def stencil_group(xs, cur, coeffs, r0):
    w01, w10, al, be, cc = coeffs
    prv = 1 - cur
    above = xs[cur, :, pl.ds(r0 - 1, SUB), :]
    mid = xs[cur, :, pl.ds(r0, SUB), :]
    below = xs[cur, :, pl.ds(r0 + 1, SUB), :]
    s = above + below
    q = al * s + w10 * mid
    r = be * (above - below)
    x = q + r
    y = q - r
    z = (w01 * s + cc * mid) - xs[prv, :, pl.ds(r0, SUB), :]
    x_wrap = pltpu.roll(x[NC - 1], 1, 1)
    y_wrap = pltpu.roll(y[0], LANES - 1, 1)
    for c in range(NC):
        xc = x[c - 1] if c else x_wrap
        yc = y[c + 1] if c < NC - 1 else y_wrap
        xs[prv, c, pl.ds(r0, SUB), :] = (z[c] + xc) + yc


def kernel(
    rows, cols, steps, kr, halo, row_n, col_n,
    u_ref, v_ref, w_hbm, now_ref, old_ref,
    w_ref, table, nu, nv, pk_l, pk_r, h_l, h_r, xs, got,
    near, in_sem, send_sem, recv_sem, edge_send, edge_recv,
):
    my_row, my_col = lax.axis_index("row"), lax.axis_index("col")
    up, down = lax.rem(my_row + row_n - 1, row_n), lax.rem(my_row + 1, row_n)
    left, right = lax.rem(my_col + col_n - 1, col_n), lax.rem(my_col + 1, col_n)
    own = pl.ds(kr, rows)
    loads = [
        pltpu.make_async_copy(u_ref, nu.at[own], in_sem.at[0]),
        pltpu.make_async_copy(v_ref, nv.at[own], in_sem.at[1]),
    ]
    load_w = pltpu.make_async_copy(w_hbm, w_ref, in_sem.at[2])
    for c in (*loads, load_w):
        c.start()
    barrier = pltpu.get_barrier_semaphore()
    around = [(my_row, left), (my_row, right), (up, my_col), (down, my_col)]
    for r, c in around:
        pl.semaphore_signal(barrier, inc=1, device_id={"row": r, "col": c}, device_id_type=MESH)
    for c in loads:
        c.wait()
    x0, x1 = xs.at[0], xs.at[1]
    lane = lane_iota()
    low = lane < halo
    nblk = cols // LANES

    def pack(g, _):
        src = pl.ds(pl.multiple_of(kr + SUB * g, SUB), SUB)
        dst = pl.ds(pl.multiple_of(SUB * g, SUB), SUB)
        u_first, v_first = nu[src, :LANES], nv[src, :LANES]
        u_last, v_last = nu[src, cols - LANES :], nv[src, cols - LANES :]
        pk_l[dst, :] = jnp.where(low, u_first, pltpu.roll(v_first, halo, 1))
        pk_r[dst, :] = jnp.where(low, pltpu.roll(v_last, halo, 1), u_last)
        return 0

    lax.fori_loop(0, rows // SUB, pack, 0, unroll=8)
    pl.semaphore_wait(barrier, len(around))
    sends = []

    def send(src, dst, r, c):
        i = len(sends)
        copy = pltpu.make_async_remote_copy(
            src_ref=src, dst_ref=dst, send_sem=send_sem.at[i], recv_sem=recv_sem.at[i],
            device_id={"row": r, "col": c}, device_id_type=MESH,
        )
        copy.start()
        sends.append(copy)

    top, bottom = pl.ds(0, kr), pl.ds(kr + rows, kr)
    half = rows // 2
    for first in (0, half):
        at = pl.ds(first, half)
        to = pl.ds(kr + first, half)
        send(pk_l.at[at], h_r.at[to], my_row, left)
        send(pk_r.at[at], h_l.at[to], my_row, right)
        if first:
            break
        for n in (nu, nv):
            send(n.at[pl.ds(kr, kr)], n.at[bottom], up, my_col)
            send(n.at[pl.ds(rows, kr)], n.at[top], down, my_col)
        for r in (up, down):
            pl.semaphore_signal(near, inc=1, device_id={"row": r}, device_id_type=MESH)
        pl.semaphore_wait(near, 2)
        send(pk_l.at[pl.ds(0, kr)], h_r.at[bottom], up, left)
        send(pk_l.at[pl.ds(rows - kr, kr)], h_r.at[top], down, left)
        send(pk_r.at[pl.ds(0, kr)], h_l.at[bottom], up, right)
        send(pk_r.at[pl.ds(rows - kr, kr)], h_l.at[top], down, right)
    residue = lax.rem(lane, NC)
    masks = [residue == m for m in range(NC)]
    base = PAD
    load_w.wait()

    def tabulate(t, _):
        for k, x in enumerate(step_coeffs(w_ref, t)):
            table[t, k] = x
        return 0

    lax.fori_loop(0, steps, tabulate, 0, unroll=4)
    for c in sends:
        c.wait()

    def unpack(g, _):
        at = pl.ds(pl.multiple_of(SUB * g, SUB), SUB)
        hl, hr = h_l[at, :], h_r[at, :]
        h_l[at, :] = jnp.where(low, hr, hl)
        h_r[at, :] = pltpu.roll(jnp.where(low, hl, hr), halo, 1)
        return 0

    groups = (rows + 2 * kr) // SUB
    lax.fori_loop(0, groups, unpack, 0, unroll=groups // 3)

    for c in range(NC):
        idx = (NC * lane + (c - halo) % LANES) & (LANES - 1)
        sel = [masks[(c - halo - LANES * b) % NC] for b in range(nblk + 1)]

        def to_lanes(g, _, c=c, idx=idx, sel=sel):
            at = pl.ds(pl.multiple_of(SUB * g, SUB), SUB)
            out = pl.ds(pl.multiple_of(base - kr + SUB * g, SUB), SUB)
            ub = [nu[at, b * LANES : (b + 1) * LANES] for b in range(nblk)] + [h_l[at, :]]
            vb = [nv[at, b * LANES : (b + 1) * LANES] for b in range(nblk)] + [h_r[at, :]]
            ul = 0.25 * permute(pick(sel, ub), idx)
            vl = permute(pick(sel, vb), idx)
            x0[c, out, :] = ul
            x1[c, out, :] = ul - 0.125 * vl
            return 0

        lax.fori_loop(0, groups, to_lanes, 0, unroll=groups // 3)

    TOP, BOTTOM = 0, 1
    cut = SUB * FIRST
    part = lax.rem(my_row, 2)
    many, fewer, other = FIRST + kr // SUB, FIRST, (rows - cut + kr) // SUB
    mid = kr // 2
    n_phase = steps // kr

    def edge_copies(side, slot):
        src = pl.ds(base + (0, rows - kr)[side], kr)
        return [
            pltpu.make_async_remote_copy(
                src_ref=x.at[:, src, :], dst_ref=got.at[1 - side, slot, i],
                send_sem=edge_send.at[side, slot, i], recv_sem=edge_recv.at[1 - side, slot, i],
                device_id={"row": (up, down)[side]}, device_id_type=MESH,
            )
            for i, x in enumerate((x0, x1))
        ]

    def take_halo(side, p):
        @pl.when(p > 0)
        def _():
            slot = lax.rem(p - 1, 2)
            for c in edge_copies(side, slot):
                c.wait_send()
            for c in edge_copies(1 - side, slot):
                c.wait_recv()
            dst = pl.ds(base + (-kr, rows)[side], kr)
            x0[:, dst, :] = got[side, slot, 0]
            x1[:, dst, :] = got[side, slot, 1]

    def send_edge(side, p):
        @pl.when(p < n_phase - 1)
        def _():
            for c in edge_copies(side, lax.rem(p, 2)):
                c.start()

    def part_steps(p, t0, count, start, sign, n):
        def some(i, _):
            for j in range(UNROLL):
                t = kr * p + t0 + UNROLL * i + j
                coeffs = [table[t, k] for k in range(5)]
                r0 = base + start + sign * (t0 + j) + sign * UNROLL * i
                for g in range(n):
                    stencil_group(xs, j % 2, coeffs, r0 + SUB * g)
            return 0

        lax.fori_loop(0, count // UNROLL, some, 0)

    def phase(p, _):
        @pl.when(part == 0)
        def _():
            take_halo(TOP, p)
            part_steps(p, 0, mid, cut - SUB * many, -1, many)
            part_steps(p, mid, kr - mid, cut - SUB * fewer, -1, fewer)
            send_edge(TOP, p)
            take_halo(BOTTOM, p)
            part_steps(p, 0, kr, cut, -1, other)
            send_edge(BOTTOM, p)

        @pl.when(part == 1)
        def _():
            take_halo(BOTTOM, p)
            part_steps(p, 0, mid, rows - cut, 1, many)
            part_steps(p, mid, kr - mid, rows - cut, 1, fewer)
            send_edge(BOTTOM, p)
            take_halo(TOP, p)
            part_steps(p, 0, kr, rows - cut - SUB * other, 1, other)
            send_edge(TOP, p)

        return 0

    lax.fori_loop(0, n_phase, phase, 0)

    inv = pow(NC, -1, LANES)
    idx = [(inv * (lane + (halo - c) % LANES)) & (LANES - 1) for c in range(NC)]

    def to_natural(g, _):
        at = pl.ds(pl.multiple_of(base + SUB * g, SUB), SUB)
        to = pl.ds(pl.multiple_of(SUB * g, SUB), SUB)
        for x, out in ((x0, now_ref), (x1, old_ref)):
            parts = [permute(x[c, at, :], idx[c]) for c in range(NC)]
            for b in range(nblk):
                sel = [masks[(c - halo - LANES * b) % NC] for c in range(NC)]
                out[to, b * LANES : (b + 1) * LANES] = pick(sel, parts)
        return 0

    lax.fori_loop(0, rows // SUB, to_natural, 0, unroll=8)


def solution(mesh):
    row_n, col_n = mesh.shape["row"], mesh.shape["col"]
    spec = P(("ens", "row"), "col")

    def local_run(u, v, w):
        rows, cols = u.shape
        steps = w.shape[0]
        kr = 2 * SUB
        halo = (NC * LANES - cols) // 2
        tall = rows + 2 * kr
        f32 = jnp.float32
        out = jax.ShapeDtypeStruct(u.shape, f32)
        now, old = pl.pallas_call(
            functools.partial(kernel, rows, cols, steps, kr, halo, row_n, col_n),
            out_shape=(out, out),
            in_specs=[
                pl.BlockSpec(memory_space=pl.ANY),
                pl.BlockSpec(memory_space=pl.ANY),
                pl.BlockSpec(memory_space=pl.ANY),
            ],
            out_specs=(pl.BlockSpec(memory_space=pltpu.VMEM), pl.BlockSpec(memory_space=pltpu.VMEM)),
            scratch_shapes=[
                pltpu.SMEM((3, 3, steps), f32),
                pltpu.VMEM((steps, 5, SUB, LANES), f32),
                pltpu.VMEM((tall, cols), f32),
                pltpu.VMEM((tall, cols), f32),
                pltpu.VMEM((rows, LANES), f32),
                pltpu.VMEM((rows, LANES), f32),
                pltpu.VMEM((tall, LANES), f32),
                pltpu.VMEM((tall, LANES), f32),
                pltpu.VMEM((2, NC, rows + 2 * PAD, LANES), f32),
                pltpu.VMEM((2, 2, 2, NC, kr, LANES), f32),
                pltpu.SemaphoreType.REGULAR,
                pltpu.SemaphoreType.DMA((3,)),
                pltpu.SemaphoreType.DMA((12,)),
                pltpu.SemaphoreType.DMA((12,)),
                pltpu.SemaphoreType.DMA((2, 2, 2)),
                pltpu.SemaphoreType.DMA((2, 2, 2)),
            ],
            compiler_params=pltpu.CompilerParams(collective_id=0, has_side_effects=True),
        )(u, v, jnp.transpose(w, (1, 2, 0)))
        return 4.0 * now, 8.0 * (now - old)

    return jax.shard_map(
        local_run, mesh=mesh, in_specs=(spec, spec, P()), out_specs=(spec, spec), check_vma=False
    )
```

```python
import functools

import jax
import jax.numpy as jnp
from jax import lax
from jax.experimental import pallas as pl
from jax.experimental.pallas import tpu as pltpu
from jax.sharding import PartitionSpec as P

LANES = 128
SUB = 8
NC = 5
UNROLL = 4
BLOCK = 2
FIRST = 12
PAD = 3 * SUB
MESH = pl.DeviceIdType.MESH


def lane_iota():
    return lax.broadcasted_iota(jnp.int32, (SUB, LANES), 1)


def permute(x, idx):
    return lax.gather(
        x, idx[..., None],
        lax.GatherDimensionNumbers(
            offset_dims=(), collapsed_slice_dims=(1,), start_index_map=(1,),
            operand_batching_dims=(0,), start_indices_batching_dims=(0,),
        ),
        slice_sizes=(1, 1), mode=lax.GatherScatterMode.PROMISE_IN_BOUNDS,
    )


def pick(masks, parts):
    out = parts[0]
    for m, p in zip(masks[1:], parts[1:]):
        out = jnp.where(m, p, out)
    return out


def step_coeffs(w_ref, t):
    w = [[jnp.full((SUB, LANES), w_ref[a, b, t]) for b in range(3)] for a in range(2)]
    return (
        0.5 * w[0][1],
        0.5 * w[1][0],
        0.25 * (w[0][0] + w[0][2]),
        0.25 * (w[0][0] - w[0][2]),
        1.5 + 0.5 * w[1][1],
    )


def stencil_rows(xs, cur, coeffs, r0):
    tall = SUB * BLOCK
    w01, w10, al, be, cc = (jnp.tile(w, (BLOCK, 1)) for w in coeffs)
    prv = 1 - cur
    above = xs[cur, :, pl.ds(r0 - 1, tall), :]
    mid = xs[cur, :, pl.ds(r0, tall), :]
    below = xs[cur, :, pl.ds(r0 + 1, tall), :]
    s = above + below
    q = al * s + w10 * mid
    r = be * (above - below)
    x = q + r
    y = q - r
    z = (w01 * s + cc * mid) - xs[prv, :, pl.ds(r0, tall), :]
    x_wrap = pltpu.roll(x[NC - 1], 1, 1)
    y_wrap = pltpu.roll(y[0], LANES - 1, 1)
    for c in range(NC):
        xc = x[c - 1] if c else x_wrap
        yc = y[c + 1] if c < NC - 1 else y_wrap
        xs[prv, c, pl.ds(r0, tall), :] = (z[c] + xc) + yc


def kernel(
    rows, cols, steps, kr, halo, row_n, col_n,
    u_ref, v_ref, w_hbm, now_ref, old_ref,
    w_ref, table, nu, nv, pk_l, pk_r, h_l, h_r, xs, got,
    near, in_sem, out_sem, send_sem, recv_sem, edge_send, edge_recv,
):
    my_row, my_col = lax.axis_index("row"), lax.axis_index("col")
    up, down = lax.rem(my_row + row_n - 1, row_n), lax.rem(my_row + 1, row_n)
    left, right = lax.rem(my_col + col_n - 1, col_n), lax.rem(my_col + 1, col_n)
    own = pl.ds(kr, rows)
    loads = [
        pltpu.make_async_copy(u_ref, nu.at[own], in_sem.at[0]),
        pltpu.make_async_copy(v_ref, nv.at[own], in_sem.at[1]),
    ]
    load_w = pltpu.make_async_copy(w_hbm, w_ref, in_sem.at[2])
    for c in (*loads, load_w):
        c.start()
    barrier = pltpu.get_barrier_semaphore()
    around = [(my_row, left), (my_row, right), (up, my_col), (down, my_col)]
    for r, c in around:
        pl.semaphore_signal(barrier, inc=1, device_id={"row": r, "col": c}, device_id_type=MESH)
    for c in loads:
        c.wait()
    x0, x1 = xs.at[0], xs.at[1]
    lane = lane_iota()
    low = lane < halo
    nblk = cols // LANES

    def pack(g, _):
        src = pl.ds(pl.multiple_of(kr + SUB * g, SUB), SUB)
        dst = pl.ds(pl.multiple_of(SUB * g, SUB), SUB)
        u_first, v_first = nu[src, :LANES], nv[src, :LANES]
        u_last, v_last = nu[src, cols - LANES :], nv[src, cols - LANES :]
        pk_l[dst, :] = jnp.where(low, u_first, pltpu.roll(v_first, halo, 1))
        pk_r[dst, :] = jnp.where(low, pltpu.roll(v_last, halo, 1), u_last)
        return 0

    lax.fori_loop(0, rows // SUB, pack, 0, unroll=8)
    pl.semaphore_wait(barrier, len(around))
    sends = []

    def send(src, dst, r, c):
        i = len(sends)
        copy = pltpu.make_async_remote_copy(
            src_ref=src, dst_ref=dst, send_sem=send_sem.at[i], recv_sem=recv_sem.at[i],
            device_id={"row": r, "col": c}, device_id_type=MESH,
        )
        copy.start()
        sends.append(copy)

    top, bottom = pl.ds(0, kr), pl.ds(kr + rows, kr)
    half = rows // 2
    for first in (0, half):
        at = pl.ds(first, half)
        to = pl.ds(kr + first, half)
        send(pk_l.at[at], h_r.at[to], my_row, left)
        send(pk_r.at[at], h_l.at[to], my_row, right)
        if first:
            break
        for n in (nu, nv):
            send(n.at[pl.ds(kr, kr)], n.at[bottom], up, my_col)
            send(n.at[pl.ds(rows, kr)], n.at[top], down, my_col)
        for r in (up, down):
            pl.semaphore_signal(near, inc=1, device_id={"row": r}, device_id_type=MESH)
        load_w.wait()

        def tabulate(t, _):
            for k, x in enumerate(step_coeffs(w_ref, t)):
                table[t, k] = x
            return 0

        lax.fori_loop(0, steps, tabulate, 0, unroll=4)
        pl.semaphore_wait(near, 2)
        send(pk_l.at[pl.ds(0, kr)], h_r.at[bottom], up, left)
        send(pk_l.at[pl.ds(rows - kr, kr)], h_r.at[top], down, left)
        send(pk_r.at[pl.ds(0, kr)], h_l.at[bottom], up, right)
        send(pk_r.at[pl.ds(rows - kr, kr)], h_l.at[top], down, right)
    residue = lax.rem(lane, NC)
    masks = [residue == m for m in range(NC)]
    base = PAD
    where_to = [
        ((NC * lane + (c - halo) % LANES) & (LANES - 1), [masks[(c - halo - LANES * b) % NC] for b in range(nblk + 1)])
        for c in range(NC)
    ]

    def to_lanes(first, count, own_only):
        for c, (idx, sel) in enumerate(where_to):
            def body(g, _, c=c, idx=idx, sel=sel):
                at = pl.ds(pl.multiple_of(first + SUB * g, SUB), SUB)
                out = pl.ds(pl.multiple_of(base - kr + first + SUB * g, SUB), SUB)
                ub = [nu[at, b * LANES : (b + 1) * LANES] for b in range(nblk)]
                vb = [nv[at, b * LANES : (b + 1) * LANES] for b in range(nblk)]
                if not own_only:
                    ub, vb = ub + [h_l[at, :]], vb + [h_r[at, :]]
                ul = 0.25 * permute(pick(sel[: len(ub)], ub), idx)
                vl = permute(pick(sel[: len(vb)], vb), idx)
                xs[0, c, out, :] = ul
                xs[1, c, out, :] = ul - 0.125 * vl
                return 0

            lax.fori_loop(0, count // SUB, body, 0, unroll=min(count // SUB, 8))

    def unpack(first, count):
        def body(g, _):
            at = pl.ds(pl.multiple_of(first + SUB * g, SUB), SUB)
            hl, hr = h_l[at, :], h_r[at, :]
            h_l[at, :] = jnp.where(low, hr, hl)
            h_r[at, :] = pltpu.roll(jnp.where(low, hl, hr), halo, 1)
            return 0

        lax.fori_loop(0, count // SUB, body, 0, unroll=min(count // SUB, 8))

    def add_halo(first, count):
        for c, (idx, _) in enumerate(where_to):
            column = NC * lane + c
            outside = (column < halo) | (column >= halo + cols)

            def body(g, _, c=c, idx=idx, outside=outside):
                at = pl.ds(pl.multiple_of(first + SUB * g, SUB), SUB)
                out = pl.ds(pl.multiple_of(base - kr + first + SUB * g, SUB), SUB)
                ul = 0.25 * permute(h_l[at, :], idx)
                vl = permute(h_r[at, :], idx)
                xs[0, c, out, :] = jnp.where(outside, ul, xs[0, c, out, :])
                xs[1, c, out, :] = jnp.where(outside, ul - 0.125 * vl, xs[1, c, out, :])
                return 0

            lax.fori_loop(0, count // SUB, body, 0, unroll=min(count // SUB, 8))

    to_lanes(kr, rows, True)
    for c in sends[:2]:
        c.wait()
    unpack(kr, half)
    add_halo(kr, half)
    for c in sends[2:]:
        c.wait()
    unpack(kr + half, half)
    add_halo(kr + half, half)
    for first in (0, kr + rows):
        unpack(first, kr)
        to_lanes(first, kr, False)

    TOP, BOTTOM = 0, 1
    cut = SUB * FIRST
    part = lax.rem(my_row, 2)
    many, fewer, other = FIRST + kr // SUB, FIRST, (rows - cut + kr) // SUB
    mid = kr // 2
    n_phase = steps // kr

    def edge_copies(side, slot):
        src = pl.ds(base + (0, rows - kr)[side], kr)
        return [
            pltpu.make_async_remote_copy(
                src_ref=x.at[:, src, :], dst_ref=got.at[1 - side, slot, i],
                send_sem=edge_send.at[side, slot, i], recv_sem=edge_recv.at[1 - side, slot, i],
                device_id={"row": (up, down)[side]}, device_id_type=MESH,
            )
            for i, x in enumerate((x0, x1))
        ]

    def take_halo(side, p):
        @pl.when(p > 0)
        def _():
            slot = lax.rem(p - 1, 2)
            for c in edge_copies(side, slot):
                c.wait_send()
            for c in edge_copies(1 - side, slot):
                c.wait_recv()
            dst = pl.ds(base + (-kr, rows)[side], kr)
            x0[:, dst, :] = got[side, slot, 0]
            x1[:, dst, :] = got[side, slot, 1]

    def send_edge(side, p):
        @pl.when(p < n_phase - 1)
        def _():
            for c in edge_copies(side, lax.rem(p, 2)):
                c.start()

    def part_steps(p, t0, count, start, sign, n):
        def some(i, _):
            for j in range(UNROLL):
                t = kr * p + t0 + UNROLL * i + j
                coeffs = [table[t, k] for k in range(5)]
                r0 = base + start + sign * (t0 + j) + sign * UNROLL * i
                for g in range(0, n, BLOCK):
                    stencil_rows(xs, j % 2, coeffs, r0 + SUB * g)
            return 0

        lax.fori_loop(0, count // UNROLL, some, 0)

    def phase(p, _):
        @pl.when(part == 0)
        def _():
            take_halo(TOP, p)
            part_steps(p, 0, mid, cut - SUB * many, -1, many)
            part_steps(p, mid, kr - mid, cut - SUB * fewer, -1, fewer)
            send_edge(TOP, p)
            take_halo(BOTTOM, p)
            part_steps(p, 0, kr, cut, -1, other)
            send_edge(BOTTOM, p)

        @pl.when(part == 1)
        def _():
            take_halo(BOTTOM, p)
            part_steps(p, 0, mid, rows - cut, 1, many)
            part_steps(p, mid, kr - mid, rows - cut, 1, fewer)
            send_edge(BOTTOM, p)
            take_halo(TOP, p)
            part_steps(p, 0, kr, rows - cut - SUB * other, 1, other)
            send_edge(TOP, p)

        return 0

    lax.fori_loop(0, n_phase, phase, 0)

    inv = pow(NC, -1, LANES)
    idx = [(inv * (lane + (halo - c) % LANES)) & (LANES - 1) for c in range(NC)]

    def to_natural(g, _):
        at = pl.ds(pl.multiple_of(base + SUB * g, SUB), SUB)
        to = pl.ds(pl.multiple_of(kr + SUB * g, SUB), SUB)
        for x, out in ((x0, nu), (x1, nv)):
            parts = [permute(x[c, at, :], idx[c]) for c in range(NC)]
            for b in range(nblk):
                sel = [masks[(c - halo - LANES * b) % NC] for c in range(NC)]
                out[to, b * LANES : (b + 1) * LANES] = pick(sel, parts)
        return 0

    stores = []
    chunk = rows // 4
    for k in range(4):
        lax.fori_loop(k * chunk // SUB, (k + 1) * chunk // SUB, to_natural, 0, unroll=8)
        for i, (x, out) in enumerate(((nu, now_ref), (nv, old_ref))):
            stores.append(
                pltpu.make_async_copy(
                    x.at[pl.ds(kr + k * chunk, chunk)], out.at[pl.ds(k * chunk, chunk)], out_sem.at[i, k]
                )
            )
            stores[-1].start()
    for c in stores:
        c.wait()


def solution(mesh):
    row_n, col_n = mesh.shape["row"], mesh.shape["col"]
    spec = P(("ens", "row"), "col")

    def local_run(u, v, w):
        rows, cols = u.shape
        steps = w.shape[0]
        kr = 2 * SUB
        halo = (NC * LANES - cols) // 2
        tall = rows + 2 * kr
        f32 = jnp.float32
        out = jax.ShapeDtypeStruct(u.shape, f32)
        now, old = pl.pallas_call(
            functools.partial(kernel, rows, cols, steps, kr, halo, row_n, col_n),
            out_shape=(out, out),
            in_specs=[
                pl.BlockSpec(memory_space=pl.ANY),
                pl.BlockSpec(memory_space=pl.ANY),
                pl.BlockSpec(memory_space=pl.ANY),
            ],
            out_specs=(pl.BlockSpec(memory_space=pl.ANY), pl.BlockSpec(memory_space=pl.ANY)),
            scratch_shapes=[
                pltpu.SMEM((3, 3, steps), f32),
                pltpu.VMEM((steps, 5, SUB, LANES), f32),
                pltpu.VMEM((tall, cols), f32),
                pltpu.VMEM((tall, cols), f32),
                pltpu.VMEM((rows, LANES), f32),
                pltpu.VMEM((rows, LANES), f32),
                pltpu.VMEM((tall, LANES), f32),
                pltpu.VMEM((tall, LANES), f32),
                pltpu.VMEM((2, NC, rows + 2 * PAD, LANES), f32),
                pltpu.VMEM((2, 2, 2, NC, kr, LANES), f32),
                pltpu.SemaphoreType.REGULAR,
                pltpu.SemaphoreType.DMA((3,)),
                pltpu.SemaphoreType.DMA((2, 4)),
                pltpu.SemaphoreType.DMA((12,)),
                pltpu.SemaphoreType.DMA((12,)),
                pltpu.SemaphoreType.DMA((2, 2, 2)),
                pltpu.SemaphoreType.DMA((2, 2, 2)),
            ],
            compiler_params=pltpu.CompilerParams(collective_id=0, has_side_effects=True),
        )(u, v, jnp.transpose(w, (1, 2, 0)))
        return 4.0 * now, 8.0 * (now - old)

    return jax.shard_map(
        local_run, mesh=mesh, in_specs=(spec, spec, P()), out_specs=(spec, spec), check_vma=False
    )
```

```python
import functools

import jax
import jax.numpy as jnp
from jax import lax
from jax.experimental import pallas as pl
from jax.experimental.pallas import tpu as pltpu
from jax.sharding import PartitionSpec as P

LANES = 128
SUB = 8
NC = 5
PIECES = 2
FIRST = 12
PAD = 3 * SUB
MESH = pl.DeviceIdType.MESH


def lane_iota():
    return lax.broadcasted_iota(jnp.int32, (SUB, LANES), 1)


def permute(x, idx):
    return lax.gather(
        x, idx[..., None],
        lax.GatherDimensionNumbers(
            offset_dims=(), collapsed_slice_dims=(1,), start_index_map=(1,),
            operand_batching_dims=(0,), start_indices_batching_dims=(0,),
        ),
        slice_sizes=(1, 1), mode=lax.GatherScatterMode.PROMISE_IN_BOUNDS,
    )


def pick(masks, parts):
    out = parts[0]
    for m, p in zip(masks[1:], parts[1:]):
        out = jnp.where(m, p, out)
    return out


def step_coeffs(w_ref, t):
    w = [[jnp.full((SUB, LANES), w_ref[a, b, t]) for b in range(3)] for a in range(2)]
    return (
        0.5 * w[0][1],
        0.5 * w[1][0],
        0.25 * (w[0][0] + w[0][2]),
        0.25 * (w[0][0] - w[0][2]),
        1.5 + 0.5 * w[1][1],
    )


def stencil_rows(xs, cur, coeffs, r0, block):
    tall = SUB * block
    w01, w10, al, be, cc = (jnp.tile(w, (block, 1)) for w in coeffs)
    prv = 1 - cur
    above = xs[cur, :, pl.ds(r0 - 1, tall), :]
    mid = xs[cur, :, pl.ds(r0, tall), :]
    below = xs[cur, :, pl.ds(r0 + 1, tall), :]
    s = above + below
    q = al * s + w10 * mid
    r = be * (above - below)
    x = q + r
    y = q - r
    z = (w01 * s + cc * mid) - xs[prv, :, pl.ds(r0, tall), :]
    x_wrap = pltpu.roll(x[NC - 1], 1, 1)
    y_wrap = pltpu.roll(y[0], LANES - 1, 1)
    for c in range(NC):
        xc = x[c - 1] if c else x_wrap
        yc = y[c + 1] if c < NC - 1 else y_wrap
        xs[prv, c, pl.ds(r0, tall), :] = (z[c] + xc) + yc


def kernel(
    rows, cols, steps, kr, halo, row_n, col_n,
    u_ref, v_ref, w_hbm, now_ref, old_ref,
    w_ref, table, nu, nv, pk_l, pk_r, h_l, h_r, xs, got,
    near, in_sem, out_sem, send_sem, recv_sem, edge_send, edge_recv,
):
    my_row, my_col = lax.axis_index("row"), lax.axis_index("col")
    up, down = lax.rem(my_row + row_n - 1, row_n), lax.rem(my_row + 1, row_n)
    left, right = lax.rem(my_col + col_n - 1, col_n), lax.rem(my_col + 1, col_n)
    own = pl.ds(kr, rows)
    loads = [
        pltpu.make_async_copy(u_ref, nu.at[own], in_sem.at[0]),
        pltpu.make_async_copy(v_ref, nv.at[own], in_sem.at[1]),
    ]
    load_w = pltpu.make_async_copy(w_hbm, w_ref, in_sem.at[2])
    for c in (*loads, load_w):
        c.start()
    barrier = pltpu.get_barrier_semaphore()
    around = [(my_row, left), (my_row, right), (up, my_col), (down, my_col)]
    for r, c in around:
        pl.semaphore_signal(barrier, inc=1, device_id={"row": r, "col": c}, device_id_type=MESH)
    for c in loads:
        c.wait()
    x0, x1 = xs.at[0], xs.at[1]
    lane = lane_iota()
    low = lane < halo
    nblk = cols // LANES

    def pack(g, _):
        src = pl.ds(pl.multiple_of(kr + SUB * g, SUB), SUB)
        dst = pl.ds(pl.multiple_of(SUB * g, SUB), SUB)
        u_first, v_first = nu[src, :LANES], nv[src, :LANES]
        u_last, v_last = nu[src, cols - LANES :], nv[src, cols - LANES :]
        pk_l[dst, :] = jnp.where(low, u_first, pltpu.roll(v_first, halo, 1))
        pk_r[dst, :] = jnp.where(low, pltpu.roll(v_last, halo, 1), u_last)
        return 0

    lax.fori_loop(0, rows // SUB, pack, 0, unroll=8)
    pl.semaphore_wait(barrier, len(around))
    sends = []

    def send(src, dst, r, c):
        i = len(sends)
        copy = pltpu.make_async_remote_copy(
            src_ref=src, dst_ref=dst, send_sem=send_sem.at[i], recv_sem=recv_sem.at[i],
            device_id={"row": r, "col": c}, device_id_type=MESH,
        )
        copy.start()
        sends.append(copy)

    top, bottom = pl.ds(0, kr), pl.ds(kr + rows, kr)
    half = rows // 2
    for first in (0, half):
        at = pl.ds(first, half)
        to = pl.ds(kr + first, half)
        send(pk_l.at[at], h_r.at[to], my_row, left)
        send(pk_r.at[at], h_l.at[to], my_row, right)
        if first:
            break
        for n in (nu, nv):
            send(n.at[pl.ds(kr, kr)], n.at[bottom], up, my_col)
            send(n.at[pl.ds(rows, kr)], n.at[top], down, my_col)
        for r in (up, down):
            pl.semaphore_signal(near, inc=1, device_id={"row": r}, device_id_type=MESH)
        load_w.wait()

        def tabulate(t, _):
            for k, x in enumerate(step_coeffs(w_ref, t)):
                table[t, k] = x
            return 0

        lax.fori_loop(0, steps, tabulate, 0, unroll=4)
        pl.semaphore_wait(near, 2)
        send(pk_l.at[pl.ds(0, kr)], h_r.at[bottom], up, left)
        send(pk_l.at[pl.ds(rows - kr, kr)], h_r.at[top], down, left)
        send(pk_r.at[pl.ds(0, kr)], h_l.at[bottom], up, right)
        send(pk_r.at[pl.ds(rows - kr, kr)], h_l.at[top], down, right)
    residue = lax.rem(lane, NC)
    masks = [residue == m for m in range(NC)]
    base = PAD
    where_to = [
        ((NC * lane + (c - halo) % LANES) & (LANES - 1), [masks[(c - halo - LANES * b) % NC] for b in range(nblk + 1)])
        for c in range(NC)
    ]

    def to_lanes(first, count, own_only):
        for c, (idx, sel) in enumerate(where_to):
            def body(g, _, c=c, idx=idx, sel=sel):
                at = pl.ds(pl.multiple_of(first + SUB * g, SUB), SUB)
                out = pl.ds(pl.multiple_of(base - kr + first + SUB * g, SUB), SUB)
                ub = [nu[at, b * LANES : (b + 1) * LANES] for b in range(nblk)]
                vb = [nv[at, b * LANES : (b + 1) * LANES] for b in range(nblk)]
                if not own_only:
                    ub, vb = ub + [h_l[at, :]], vb + [h_r[at, :]]
                ul = 0.25 * permute(pick(sel[: len(ub)], ub), idx)
                vl = permute(pick(sel[: len(vb)], vb), idx)
                xs[0, c, out, :] = ul
                xs[1, c, out, :] = ul - 0.125 * vl
                return 0

            lax.fori_loop(0, count // SUB, body, 0, unroll=min(count // SUB, 8))

    def unpack(first, count):
        def body(g, _):
            at = pl.ds(pl.multiple_of(first + SUB * g, SUB), SUB)
            hl, hr = h_l[at, :], h_r[at, :]
            h_l[at, :] = jnp.where(low, hr, hl)
            h_r[at, :] = pltpu.roll(jnp.where(low, hl, hr), halo, 1)
            return 0

        lax.fori_loop(0, count // SUB, body, 0, unroll=min(count // SUB, 8))

    def add_halo(first, count):
        for c, (idx, _) in enumerate(where_to):
            column = NC * lane + c
            outside = (column < halo) | (column >= halo + cols)

            def body(g, _, c=c, idx=idx, outside=outside):
                at = pl.ds(pl.multiple_of(first + SUB * g, SUB), SUB)
                out = pl.ds(pl.multiple_of(base - kr + first + SUB * g, SUB), SUB)
                ul = 0.25 * permute(h_l[at, :], idx)
                vl = permute(h_r[at, :], idx)
                xs[0, c, out, :] = jnp.where(outside, ul, xs[0, c, out, :])
                xs[1, c, out, :] = jnp.where(outside, ul - 0.125 * vl, xs[1, c, out, :])
                return 0

            lax.fori_loop(0, count // SUB, body, 0, unroll=min(count // SUB, 8))

    to_lanes(kr, rows, True)
    for c in sends[:2]:
        c.wait()
    unpack(kr, half)
    add_halo(kr, half)
    for c in sends[2:]:
        c.wait()
    unpack(kr + half, half)
    add_halo(kr + half, half)
    for first in (0, kr + rows):
        unpack(first, kr)
        to_lanes(first, kr, False)

    TOP, BOTTOM = 0, 1
    cut = SUB * FIRST
    part = lax.rem(my_row, 2)
    n_phase = steps // kr

    def edge_copies(side, slot):
        src = pl.ds(base + (0, rows - kr)[side], kr)
        return [
            pltpu.make_async_remote_copy(
                src_ref=x.at[:, src, :], dst_ref=got.at[1 - side, slot, i],
                send_sem=edge_send.at[side, slot, i], recv_sem=edge_recv.at[1 - side, slot, i],
                device_id={"row": (up, down)[side]}, device_id_type=MESH,
            )
            for i, x in enumerate((x0, x1))
        ]

    def take_halo(side, p):
        @pl.when(p > 0)
        def _():
            slot = lax.rem(p - 1, 2)
            for c in edge_copies(side, slot):
                c.wait_send()
            for c in edge_copies(1 - side, slot):
                c.wait_recv()
            dst = pl.ds(base + (-kr, rows)[side], kr)
            x0[:, dst, :] = got[side, slot, 0]
            x1[:, dst, :] = got[side, slot, 1]

    def send_edge(side, p):
        @pl.when(p < n_phase - 1)
        def _():
            for c in edge_copies(side, lax.rem(p, 2)):
                c.start()

    def part_steps(p, first_part, sign):
        for t in range(kr):
            rows_needed = cut + kr - 1 - 2 * t if first_part else rows - cut + kr - 1
            n = -(-rows_needed // SUB)
            at_cut = cut if sign < 0 else rows - cut
            below_cut = first_part == (sign < 0)
            start = base + at_cut + sign * t - (SUB * n if below_cut else 0)
            coeffs = [table[kr * p + t, k] for k in range(5)]
            block = -(-n // PIECES)
            for g in range(0, n, block):
                stencil_rows(xs, t % 2, coeffs, start + SUB * g, min(block, n - g))

    def phase(p, _):
        @pl.when(part == 0)
        def _():
            take_halo(TOP, p)
            part_steps(p, True, -1)
            send_edge(TOP, p)
            take_halo(BOTTOM, p)
            part_steps(p, False, -1)
            send_edge(BOTTOM, p)

        @pl.when(part == 1)
        def _():
            take_halo(BOTTOM, p)
            part_steps(p, True, 1)
            send_edge(BOTTOM, p)
            take_halo(TOP, p)
            part_steps(p, False, 1)
            send_edge(TOP, p)

        return 0

    lax.fori_loop(0, n_phase, phase, 0)

    inv = pow(NC, -1, LANES)
    idx = [(inv * (lane + (halo - c) % LANES)) & (LANES - 1) for c in range(NC)]

    def to_natural(g, _):
        at = pl.ds(pl.multiple_of(base + SUB * g, SUB), SUB)
        to = pl.ds(pl.multiple_of(kr + SUB * g, SUB), SUB)
        for x, out in ((x0, nu), (x1, nv)):
            parts = [permute(x[c, at, :], idx[c]) for c in range(NC)]
            for b in range(nblk):
                sel = [masks[(c - halo - LANES * b) % NC] for c in range(NC)]
                out[to, b * LANES : (b + 1) * LANES] = pick(sel, parts)
        return 0

    stores = []
    chunk = rows // 4
    for k in range(4):
        lax.fori_loop(k * chunk // SUB, (k + 1) * chunk // SUB, to_natural, 0, unroll=8)
        for i, (x, out) in enumerate(((nu, now_ref), (nv, old_ref))):
            stores.append(
                pltpu.make_async_copy(
                    x.at[pl.ds(kr + k * chunk, chunk)], out.at[pl.ds(k * chunk, chunk)], out_sem.at[i, k]
                )
            )
            stores[-1].start()
    for c in stores:
        c.wait()


def solution(mesh):
    row_n, col_n = mesh.shape["row"], mesh.shape["col"]
    spec = P(("ens", "row"), "col")

    def local_run(u, v, w):
        rows, cols = u.shape
        steps = w.shape[0]
        kr = 2 * SUB
        halo = (NC * LANES - cols) // 2
        tall = rows + 2 * kr
        f32 = jnp.float32
        out = jax.ShapeDtypeStruct(u.shape, f32)
        now, old = pl.pallas_call(
            functools.partial(kernel, rows, cols, steps, kr, halo, row_n, col_n),
            out_shape=(out, out),
            in_specs=[
                pl.BlockSpec(memory_space=pl.ANY),
                pl.BlockSpec(memory_space=pl.ANY),
                pl.BlockSpec(memory_space=pl.ANY),
            ],
            out_specs=(pl.BlockSpec(memory_space=pl.ANY), pl.BlockSpec(memory_space=pl.ANY)),
            scratch_shapes=[
                pltpu.SMEM((3, 3, steps), f32),
                pltpu.VMEM((steps, 5, SUB, LANES), f32),
                pltpu.VMEM((tall, cols), f32),
                pltpu.VMEM((tall, cols), f32),
                pltpu.VMEM((rows, LANES), f32),
                pltpu.VMEM((rows, LANES), f32),
                pltpu.VMEM((tall, LANES), f32),
                pltpu.VMEM((tall, LANES), f32),
                pltpu.VMEM((2, NC, rows + 2 * PAD, LANES), f32),
                pltpu.VMEM((2, 2, 2, NC, kr, LANES), f32),
                pltpu.SemaphoreType.REGULAR,
                pltpu.SemaphoreType.DMA((3,)),
                pltpu.SemaphoreType.DMA((2, 4)),
                pltpu.SemaphoreType.DMA((12,)),
                pltpu.SemaphoreType.DMA((12,)),
                pltpu.SemaphoreType.DMA((2, 2, 2)),
                pltpu.SemaphoreType.DMA((2, 2, 2)),
            ],
            compiler_params=pltpu.CompilerParams(collective_id=0, has_side_effects=True),
        )(u, v, jnp.transpose(w, (1, 2, 0)))
        return 4.0 * now, 8.0 * (now - old)

    return jax.shard_map(
        local_run, mesh=mesh, in_specs=(spec, spec, P()), out_specs=(spec, spec), check_vma=False
    )
```

```python
import functools

import jax
import jax.numpy as jnp
from jax import lax
from jax.experimental import pallas as pl
from jax.experimental.pallas import tpu as pltpu
from jax.sharding import PartitionSpec as P

LANES = 128
SUB = 8
NC = 5
PIECES = 2
FIRST = 12
PAD = 3 * SUB
MESH = pl.DeviceIdType.MESH


def unroll_of(n):
    return max(k for k in range(1, 10) if n % k == 0)


def lane_iota():
    return lax.broadcasted_iota(jnp.int32, (SUB, LANES), 1)


def permute(x, idx):
    return lax.gather(
        x, idx[..., None],
        lax.GatherDimensionNumbers(
            offset_dims=(), collapsed_slice_dims=(1,), start_index_map=(1,),
            operand_batching_dims=(0,), start_indices_batching_dims=(0,),
        ),
        slice_sizes=(1, 1), mode=lax.GatherScatterMode.PROMISE_IN_BOUNDS,
    )


def pick(masks, parts):
    out = parts[0]
    for m, p in zip(masks[1:], parts[1:]):
        out = jnp.where(m, p, out)
    return out


def step_coeffs(w_ref, t):
    w = [[jnp.full((SUB, LANES), w_ref[a, b, t]) for b in range(3)] for a in range(2)]
    return (
        0.5 * w[0][1],
        0.5 * w[1][0],
        0.25 * (w[0][0] + w[0][2]),
        0.25 * (w[0][0] - w[0][2]),
        1.5 + 0.5 * w[1][1],
    )


def stencil_rows(xs, cur, coeffs, r0, block):
    tall = SUB * block
    w01, w10, al, be, cc = (jnp.tile(w, (block, 1)) for w in coeffs)
    prv = 1 - cur
    above = xs[cur, :, pl.ds(r0 - 1, tall), :]
    mid = xs[cur, :, pl.ds(r0, tall), :]
    below = xs[cur, :, pl.ds(r0 + 1, tall), :]
    s = above + below
    q = al * s + w10 * mid
    r = be * (above - below)
    x = q + r
    y = q - r
    z = (w01 * s + cc * mid) - xs[prv, :, pl.ds(r0, tall), :]
    x_wrap = pltpu.roll(x[NC - 1], 1, 1)
    y_wrap = pltpu.roll(y[0], LANES - 1, 1)
    for c in range(NC):
        xc = x[c - 1] if c else x_wrap
        yc = y[c + 1] if c < NC - 1 else y_wrap
        xs[prv, c, pl.ds(r0, tall), :] = (z[c] + xc) + yc


def kernel(
    rows, cols, steps, kr, halo, row_n, col_n,
    u_ref, v_ref, w_hbm, now_ref, old_ref,
    w_ref, table, nu, nv, pk_l, pk_r, h_l, h_r, xs, got,
    near, in_sem, out_sem, send_sem, recv_sem, edge_send, edge_recv,
):
    my_row, my_col = lax.axis_index("row"), lax.axis_index("col")
    up, down = lax.rem(my_row + row_n - 1, row_n), lax.rem(my_row + 1, row_n)
    left, right = lax.rem(my_col + col_n - 1, col_n), lax.rem(my_col + 1, col_n)
    own = pl.ds(kr, rows)
    loads = [
        pltpu.make_async_copy(u_ref, nu.at[own], in_sem.at[0]),
        pltpu.make_async_copy(v_ref, nv.at[own], in_sem.at[1]),
    ]
    load_w = pltpu.make_async_copy(w_hbm, w_ref, in_sem.at[2])
    for c in (*loads, load_w):
        c.start()
    barrier = pltpu.get_barrier_semaphore()
    around = [(my_row, left), (my_row, right), (up, my_col), (down, my_col)]
    for r, c in around:
        pl.semaphore_signal(barrier, inc=1, device_id={"row": r, "col": c}, device_id_type=MESH)
    for c in loads:
        c.wait()
    x0, x1 = xs.at[0], xs.at[1]
    lane = lane_iota()
    low = lane < halo
    nblk = cols // LANES

    def pack(g, _):
        src = pl.ds(pl.multiple_of(kr + SUB * g, SUB), SUB)
        dst = pl.ds(pl.multiple_of(SUB * g, SUB), SUB)
        u_first, v_first = nu[src, :LANES], nv[src, :LANES]
        u_last, v_last = nu[src, cols - LANES :], nv[src, cols - LANES :]
        pk_l[dst, :] = jnp.where(low, u_first, pltpu.roll(v_first, halo, 1))
        pk_r[dst, :] = jnp.where(low, pltpu.roll(v_last, halo, 1), u_last)
        return 0

    lax.fori_loop(0, rows // SUB, pack, 0, unroll=8)
    pl.semaphore_wait(barrier, len(around))
    for r in (up, down):
        pl.semaphore_signal(near, inc=1, device_id={"row": r}, device_id_type=MESH)
    sends = []

    def send(src, dst, r, c):
        i = len(sends)
        copy = pltpu.make_async_remote_copy(
            src_ref=src, dst_ref=dst, send_sem=send_sem.at[i], recv_sem=recv_sem.at[i],
            device_id={"row": r, "col": c}, device_id_type=MESH,
        )
        copy.start()
        sends.append(copy)

    top, bottom = pl.ds(0, kr), pl.ds(kr + rows, kr)
    TOP, BOTTOM = 0, 1
    part = lax.rem(my_row, 2)
    cut = SUB * FIRST
    early_rows = cut + kr
    late_rows = rows - early_rows
    early_at, late_at = part * late_rows, (1 - part) * early_rows
    landing = {TOP: [], BOTTOM: []}

    def send_columns(first, count):
        at = pl.ds(pl.multiple_of(first, SUB), count)
        to = pl.ds(pl.multiple_of(kr + first, SUB), count)
        send(pk_l.at[at], h_r.at[to], my_row, left)
        send(pk_r.at[at], h_l.at[to], my_row, right)
        return sends[-2:]

    early = send_columns(early_at, early_rows)
    for n in (nu, nv):
        send(n.at[pl.ds(kr, kr)], n.at[bottom], up, my_col)
        landing[BOTTOM].append(sends[-1])
        send(n.at[pl.ds(rows, kr)], n.at[top], down, my_col)
        landing[TOP].append(sends[-1])
    load_w.wait()

    def tabulate(t, _):
        for k, x in enumerate(step_coeffs(w_ref, t)):
            table[t, k] = x
        return 0

    lax.fori_loop(0, steps, tabulate, 0, unroll=4)
    pl.semaphore_wait(near, 2)
    for pk, h, c in ((pk_l, h_r, left), (pk_r, h_l, right)):
        send(pk.at[pl.ds(0, kr)], h.at[bottom], up, c)
        landing[BOTTOM].append(sends[-1])
        send(pk.at[pl.ds(rows - kr, kr)], h.at[top], down, c)
        landing[TOP].append(sends[-1])
    late = send_columns(late_at, late_rows)
    residue = lax.rem(lane, NC)
    masks = [residue == m for m in range(NC)]
    base = PAD
    where_to = [
        ((NC * lane + (c - halo) % LANES) & (LANES - 1), [masks[(c - halo - LANES * b) % NC] for b in range(nblk + 1)])
        for c in range(NC)
    ]

    def to_lanes(first, count, own_only):
        for c, (idx, sel) in enumerate(where_to):
            def body(g, _, c=c, idx=idx, sel=sel):
                at = pl.ds(pl.multiple_of(first + SUB * g, SUB), SUB)
                out = pl.ds(pl.multiple_of(base - kr + first + SUB * g, SUB), SUB)
                ub = [nu[at, b * LANES : (b + 1) * LANES] for b in range(nblk)]
                vb = [nv[at, b * LANES : (b + 1) * LANES] for b in range(nblk)]
                if not own_only:
                    ub, vb = ub + [h_l[at, :]], vb + [h_r[at, :]]
                ul = 0.25 * permute(pick(sel[: len(ub)], ub), idx)
                vl = permute(pick(sel[: len(vb)], vb), idx)
                xs[0, c, out, :] = ul
                xs[1, c, out, :] = ul - 0.125 * vl
                return 0

            lax.fori_loop(0, count // SUB, body, 0, unroll=unroll_of(count // SUB))

    def unpack(first, count):
        def body(g, _):
            at = pl.ds(pl.multiple_of(first + SUB * g, SUB), SUB)
            hl, hr = h_l[at, :], h_r[at, :]
            h_l[at, :] = jnp.where(low, hr, hl)
            h_r[at, :] = pltpu.roll(jnp.where(low, hl, hr), halo, 1)
            return 0

        lax.fori_loop(0, count // SUB, body, 0, unroll=unroll_of(count // SUB))

    def add_halo(first, count):
        for c, (idx, _) in enumerate(where_to):
            column = NC * lane + c
            outside = (column < halo) | (column >= halo + cols)

            def body(g, _, c=c, idx=idx, outside=outside):
                at = pl.ds(pl.multiple_of(first + SUB * g, SUB), SUB)
                out = pl.ds(pl.multiple_of(base - kr + first + SUB * g, SUB), SUB)
                ul = 0.25 * permute(h_l[at, :], idx)
                vl = permute(h_r[at, :], idx)
                xs[0, c, out, :] = jnp.where(outside, ul, xs[0, c, out, :])
                xs[1, c, out, :] = jnp.where(outside, ul - 0.125 * vl, xs[1, c, out, :])
                return 0

            lax.fori_loop(0, count // SUB, body, 0, unroll=unroll_of(count // SUB))

    def take_columns(copies, first, count):
        for c in copies:
            c.wait()
        unpack(kr + first, count)
        add_halo(kr + first, count)

    def take_rows(side):
        for c in landing[side]:
            c.wait()
        first = (0, kr + rows)[side]
        unpack(first, kr)
        to_lanes(first, kr, False)

    to_lanes(kr, rows, True)
    take_columns(early, early_at, early_rows)
    for side in (TOP, BOTTOM):
        pl.when(part == side)(functools.partial(take_rows, side))

    n_phase = steps // kr

    def edge_copies(side, slot):
        src = pl.ds(base + (0, rows - kr)[side], kr)
        return [
            pltpu.make_async_remote_copy(
                src_ref=x.at[:, src, :], dst_ref=got.at[1 - side, slot, i],
                send_sem=edge_send.at[side, slot, i], recv_sem=edge_recv.at[1 - side, slot, i],
                device_id={"row": (up, down)[side]}, device_id_type=MESH,
            )
            for i, x in enumerate((x0, x1))
        ]

    def take_halo(side, p):
        @pl.when(p > 0)
        def _():
            slot = lax.rem(p - 1, 2)
            for c in edge_copies(side, slot):
                c.wait_send()
            for c in edge_copies(1 - side, slot):
                c.wait_recv()
            dst = pl.ds(base + (-kr, rows)[side], kr)
            x0[:, dst, :] = got[side, slot, 0]
            x1[:, dst, :] = got[side, slot, 1]

    def send_edge(side, p):
        @pl.when(p < n_phase - 1)
        def _():
            for c in edge_copies(side, lax.rem(p, 2)):
                c.start()

    def part_steps(p, first_part, sign):
        for t in range(kr):
            rows_needed = cut + kr - 1 - 2 * t if first_part else rows - cut + kr - 1
            n = -(-rows_needed // SUB)
            at_cut = cut if sign < 0 else rows - cut
            below_cut = first_part == (sign < 0)
            start = base + at_cut + sign * t - (SUB * n if below_cut else 0)
            coeffs = [table[kr * p + t, k] for k in range(5)]
            block = -(-n // PIECES)
            for g in range(0, n, block):
                stencil_rows(xs, t % 2, coeffs, start + SUB * g, min(block, n - g))

    def take_late(side, p):
        @pl.when(p == 0)
        def _():
            take_columns(late, (early_rows, 0)[1 - side], late_rows)
            take_rows(side)

    def phase(p, _):
        @pl.when(part == 0)
        def _():
            take_halo(TOP, p)
            part_steps(p, True, -1)
            send_edge(TOP, p)
            take_late(BOTTOM, p)
            take_halo(BOTTOM, p)
            part_steps(p, False, -1)
            send_edge(BOTTOM, p)

        @pl.when(part == 1)
        def _():
            take_halo(BOTTOM, p)
            part_steps(p, True, 1)
            send_edge(BOTTOM, p)
            take_late(TOP, p)
            take_halo(TOP, p)
            part_steps(p, False, 1)
            send_edge(TOP, p)

        return 0

    lax.fori_loop(0, n_phase, phase, 0)

    inv = pow(NC, -1, LANES)
    idx = [(inv * (lane + (halo - c) % LANES)) & (LANES - 1) for c in range(NC)]

    wide = 4
    def to_natural(g, _):
        ats = [pl.multiple_of(SUB * (wide * g + k), SUB) for k in range(wide)]
        parts = {}
        for c in range(NC):
            for k in range(wide):
                for i in range(2):
                    parts[i, k, c] = permute(xs[i, c, pl.ds(base + ats[k], SUB), :], idx[c])
        for k in range(wide):
            for i, out in enumerate((nu, nv)):
                for b in range(nblk):
                    sel = [masks[(c - halo - LANES * b) % NC] for c in range(NC)]
                    out[pl.ds(kr + ats[k], SUB), b * LANES : (b + 1) * LANES] = pick(
                        sel, [parts[i, k, c] for c in range(NC)]
                    )
        return 0

    stores = []
    chunk = rows // 4
    for k in range(4):
        lax.fori_loop(k * chunk // (SUB * wide), (k + 1) * chunk // (SUB * wide), to_natural, 0, unroll=2)
        for i, (x, out) in enumerate(((nu, now_ref), (nv, old_ref))):
            stores.append(
                pltpu.make_async_copy(
                    x.at[pl.ds(kr + k * chunk, chunk)], out.at[pl.ds(k * chunk, chunk)], out_sem.at[i, k]
                )
            )
            stores[-1].start()
    for c in stores:
        c.wait()


def solution(mesh):
    row_n, col_n = mesh.shape["row"], mesh.shape["col"]
    spec = P(("ens", "row"), "col")

    def local_run(u, v, w):
        rows, cols = u.shape
        steps = w.shape[0]
        kr = 2 * SUB
        halo = (NC * LANES - cols) // 2
        tall = rows + 2 * kr
        f32 = jnp.float32
        out = jax.ShapeDtypeStruct(u.shape, f32)
        now, old = pl.pallas_call(
            functools.partial(kernel, rows, cols, steps, kr, halo, row_n, col_n),
            out_shape=(out, out),
            in_specs=[
                pl.BlockSpec(memory_space=pl.ANY),
                pl.BlockSpec(memory_space=pl.ANY),
                pl.BlockSpec(memory_space=pl.ANY),
            ],
            out_specs=(pl.BlockSpec(memory_space=pl.ANY), pl.BlockSpec(memory_space=pl.ANY)),
            scratch_shapes=[
                pltpu.SMEM((3, 3, steps), f32),
                pltpu.VMEM((steps, 5, SUB, LANES), f32),
                pltpu.VMEM((tall, cols), f32),
                pltpu.VMEM((tall, cols), f32),
                pltpu.VMEM((rows, LANES), f32),
                pltpu.VMEM((rows, LANES), f32),
                pltpu.VMEM((tall, LANES), f32),
                pltpu.VMEM((tall, LANES), f32),
                pltpu.VMEM((2, NC, rows + 2 * PAD, LANES), f32),
                pltpu.VMEM((2, 2, 2, NC, kr, LANES), f32),
                pltpu.SemaphoreType.REGULAR,
                pltpu.SemaphoreType.DMA((3,)),
                pltpu.SemaphoreType.DMA((2, 4)),
                pltpu.SemaphoreType.DMA((12,)),
                pltpu.SemaphoreType.DMA((12,)),
                pltpu.SemaphoreType.DMA((2, 2, 2)),
                pltpu.SemaphoreType.DMA((2, 2, 2)),
            ],
            compiler_params=pltpu.CompilerParams(collective_id=0, has_side_effects=True),
        )(u, v, jnp.transpose(w, (1, 2, 0)))
        return 4.0 * now, 8.0 * (now - old)

    return jax.shard_map(
        local_run, mesh=mesh, in_specs=(spec, spec, P()), out_specs=(spec, spec), check_vma=False
    )
```

```python
import functools

import jax
import jax.numpy as jnp
from jax import lax
from jax.experimental import pallas as pl
from jax.experimental.pallas import tpu as pltpu
from jax.sharding import PartitionSpec as P

LANES = 128
SUB = 8
NC = 5
PIECES = 2
FIRST = 12
PAD = 3 * SUB
MESH = pl.DeviceIdType.MESH


def unroll_of(n):
    return max(k for k in range(1, 10) if n % k == 0)


def lane_iota():
    return lax.broadcasted_iota(jnp.int32, (SUB, LANES), 1)


def permute(x, idx):
    return lax.gather(
        x, idx[..., None],
        lax.GatherDimensionNumbers(
            offset_dims=(), collapsed_slice_dims=(1,), start_index_map=(1,),
            operand_batching_dims=(0,), start_indices_batching_dims=(0,),
        ),
        slice_sizes=(1, 1), mode=lax.GatherScatterMode.PROMISE_IN_BOUNDS,
    )


def pick(masks, parts):
    out = parts[0]
    for m, p in zip(masks[1:], parts[1:]):
        out = jnp.where(m, p, out)
    return out


def step_coeffs(w_ref, t):
    w = [[jnp.full((SUB, LANES), w_ref[a, b, t]) for b in range(3)] for a in range(2)]
    return (
        0.5 * w[0][1],
        0.5 * w[1][0],
        0.25 * (w[0][0] + w[0][2]),
        0.25 * (w[0][0] - w[0][2]),
        1.5 + 0.5 * w[1][1],
    )


def stencil_rows(xs, cur, coeffs, r0, block):
    tall = SUB * block
    w01, w10, al, be, cc = (jnp.tile(w, (block, 1)) for w in coeffs)
    prv = 1 - cur
    above = xs[cur, :, pl.ds(r0 - 1, tall), :]
    mid = xs[cur, :, pl.ds(r0, tall), :]
    below = xs[cur, :, pl.ds(r0 + 1, tall), :]
    s = above + below
    q = al * s + w10 * mid
    r = be * (above - below)
    x = q + r
    y = q - r
    z = (w01 * s + cc * mid) - xs[prv, :, pl.ds(r0, tall), :]
    x_wrap = pltpu.roll(x[NC - 1], 1, 1)
    y_wrap = pltpu.roll(y[0], LANES - 1, 1)
    for c in range(NC):
        xc = x[c - 1] if c else x_wrap
        yc = y[c + 1] if c < NC - 1 else y_wrap
        xs[prv, c, pl.ds(r0, tall), :] = (z[c] + xc) + yc


def kernel(
    rows, cols, steps, kr, halo, row_n, col_n,
    u_ref, v_ref, w_hbm, now_ref, old_ref,
    w_ref, table, nu, nv, pk_l, pk_r, h_l, h_r, xs, got,
    near, in_sem, out_sem, send_sem, recv_sem, edge_send, edge_recv,
):
    my_row, my_col = lax.axis_index("row"), lax.axis_index("col")
    up, down = lax.rem(my_row + row_n - 1, row_n), lax.rem(my_row + 1, row_n)
    left, right = lax.rem(my_col + col_n - 1, col_n), lax.rem(my_col + 1, col_n)
    own = pl.ds(kr, rows)
    loads = [
        pltpu.make_async_copy(u_ref, nu.at[own], in_sem.at[0]),
        pltpu.make_async_copy(v_ref, nv.at[own], in_sem.at[1]),
    ]
    load_w = pltpu.make_async_copy(w_hbm, w_ref, in_sem.at[2])
    for c in (*loads, load_w):
        c.start()
    barrier = pltpu.get_barrier_semaphore()
    around = [(my_row, left), (my_row, right), (up, my_col), (down, my_col)]
    for r, c in around:
        pl.semaphore_signal(barrier, inc=1, device_id={"row": r, "col": c}, device_id_type=MESH)
    for c in loads:
        c.wait()
    x0, x1 = xs.at[0], xs.at[1]
    lane = lane_iota()
    low = lane < halo
    nblk = cols // LANES

    def pack(g, _):
        src = pl.ds(pl.multiple_of(kr + SUB * g, SUB), SUB)
        dst = pl.ds(pl.multiple_of(SUB * g, SUB), SUB)
        u_first, v_first = nu[src, :LANES], nv[src, :LANES]
        u_last, v_last = nu[src, cols - LANES :], nv[src, cols - LANES :]
        pk_l[dst, :] = jnp.where(low, u_first, pltpu.roll(v_first, halo, 1))
        pk_r[dst, :] = jnp.where(low, pltpu.roll(v_last, halo, 1), u_last)
        return 0

    lax.fori_loop(0, rows // SUB, pack, 0, unroll=8)
    pl.semaphore_wait(barrier, len(around))
    for r in (up, down):
        pl.semaphore_signal(near, inc=1, device_id={"row": r}, device_id_type=MESH)
    sends = []

    def send(src, dst, r, c):
        i = len(sends)
        copy = pltpu.make_async_remote_copy(
            src_ref=src, dst_ref=dst, send_sem=send_sem.at[i], recv_sem=recv_sem.at[i],
            device_id={"row": r, "col": c}, device_id_type=MESH,
        )
        copy.start()
        sends.append(copy)

    top, bottom = pl.ds(0, kr), pl.ds(kr + rows, kr)
    TOP, BOTTOM = 0, 1
    part = lax.rem(my_row, 2)
    cut = SUB * FIRST
    early_rows = cut + kr
    late_rows = rows - early_rows
    early_at, late_at = part * late_rows, (1 - part) * early_rows
    landing = {TOP: [], BOTTOM: []}

    def send_columns(first, count):
        at = pl.ds(pl.multiple_of(first, SUB), count)
        to = pl.ds(pl.multiple_of(kr + first, SUB), count)
        send(pk_l.at[at], h_r.at[to], my_row, left)
        send(pk_r.at[at], h_l.at[to], my_row, right)
        return sends[-2:]

    early = send_columns(early_at, early_rows)
    load_w.wait()

    def tabulate(t, _):
        for k, x in enumerate(step_coeffs(w_ref, t)):
            table[t, k] = x
        return 0

    lax.fori_loop(0, steps, tabulate, 0, unroll=4)
    pl.semaphore_wait(near, 2)
    for pk, h, c in ((pk_l, h_r, left), (pk_r, h_l, right)):
        send(pk.at[pl.ds(0, kr)], h.at[bottom], up, c)
        landing[BOTTOM].append(sends[-1])
        send(pk.at[pl.ds(rows - kr, kr)], h.at[top], down, c)
        landing[TOP].append(sends[-1])
    for n in (nu, nv):
        send(n.at[pl.ds(kr, kr)], n.at[bottom], up, my_col)
        landing[BOTTOM].append(sends[-1])
        send(n.at[pl.ds(rows, kr)], n.at[top], down, my_col)
        landing[TOP].append(sends[-1])
    late = send_columns(late_at, late_rows)
    residue = lax.rem(lane, NC)
    masks = [residue == m for m in range(NC)]
    base = PAD
    where_to = [
        ((NC * lane + (c - halo) % LANES) & (LANES - 1), [masks[(c - halo - LANES * b) % NC] for b in range(nblk + 1)])
        for c in range(NC)
    ]

    def to_lanes(first, count, own_only):
        for c, (idx, sel) in enumerate(where_to):
            def body(g, _, c=c, idx=idx, sel=sel):
                at = pl.ds(pl.multiple_of(first + SUB * g, SUB), SUB)
                out = pl.ds(pl.multiple_of(base - kr + first + SUB * g, SUB), SUB)
                ub = [nu[at, b * LANES : (b + 1) * LANES] for b in range(nblk)]
                vb = [nv[at, b * LANES : (b + 1) * LANES] for b in range(nblk)]
                if not own_only:
                    ub, vb = ub + [h_l[at, :]], vb + [h_r[at, :]]
                ul = 0.25 * permute(pick(sel[: len(ub)], ub), idx)
                vl = permute(pick(sel[: len(vb)], vb), idx)
                xs[0, c, out, :] = ul
                xs[1, c, out, :] = ul - 0.125 * vl
                return 0

            lax.fori_loop(0, count // SUB, body, 0, unroll=unroll_of(count // SUB))

    def unpack(first, count):
        def body(g, _):
            at = pl.ds(pl.multiple_of(first + SUB * g, SUB), SUB)
            hl, hr = h_l[at, :], h_r[at, :]
            h_l[at, :] = jnp.where(low, hr, hl)
            h_r[at, :] = pltpu.roll(jnp.where(low, hl, hr), halo, 1)
            return 0

        lax.fori_loop(0, count // SUB, body, 0, unroll=unroll_of(count // SUB))

    def add_halo(first, count):
        for c, (idx, _) in enumerate(where_to):
            column = NC * lane + c
            outside = (column < halo) | (column >= halo + cols)

            def body(g, _, c=c, idx=idx, outside=outside):
                at = pl.ds(pl.multiple_of(first + SUB * g, SUB), SUB)
                out = pl.ds(pl.multiple_of(base - kr + first + SUB * g, SUB), SUB)
                ul = 0.25 * permute(h_l[at, :], idx)
                vl = permute(h_r[at, :], idx)
                xs[0, c, out, :] = jnp.where(outside, ul, xs[0, c, out, :])
                xs[1, c, out, :] = jnp.where(outside, ul - 0.125 * vl, xs[1, c, out, :])
                return 0

            lax.fori_loop(0, count // SUB, body, 0, unroll=unroll_of(count // SUB))

    def take_columns(copies, first, count):
        for c in copies:
            c.wait()
        unpack(kr + first, count)
        add_halo(kr + first, count)

    def take_rows(side):
        for c in landing[side]:
            c.wait()
        first = (0, kr + rows)[side]
        unpack(first, kr)
        to_lanes(first, kr, False)

    to_lanes(kr, rows, True)
    take_columns(early, early_at, early_rows)
    for side in (TOP, BOTTOM):
        pl.when(part == side)(functools.partial(take_rows, side))

    n_phase = steps // kr

    def edge_copies(side, slot):
        src = pl.ds(base + (0, rows - kr)[side], kr)
        return [
            pltpu.make_async_remote_copy(
                src_ref=x.at[:, src, :], dst_ref=got.at[1 - side, slot, i],
                send_sem=edge_send.at[side, slot, i], recv_sem=edge_recv.at[1 - side, slot, i],
                device_id={"row": (up, down)[side]}, device_id_type=MESH,
            )
            for i, x in enumerate((x0, x1))
        ]

    def take_halo(side, p):
        @pl.when(p > 0)
        def _():
            slot = lax.rem(p - 1, 2)
            for c in edge_copies(side, slot):
                c.wait_send()
            for c in edge_copies(1 - side, slot):
                c.wait_recv()
            dst = pl.ds(base + (-kr, rows)[side], kr)
            x0[:, dst, :] = got[side, slot, 0]
            x1[:, dst, :] = got[side, slot, 1]

    def send_edge(side, p):
        @pl.when(p < n_phase - 1)
        def _():
            for c in edge_copies(side, lax.rem(p, 2)):
                c.start()

    def part_steps(p, first_part, sign):
        for t in range(kr):
            rows_needed = cut + kr - 1 - 2 * t if first_part else rows - cut + kr - 1
            n = -(-rows_needed // SUB)
            at_cut = cut if sign < 0 else rows - cut
            below_cut = first_part == (sign < 0)
            start = base + at_cut + sign * t - (SUB * n if below_cut else 0)
            coeffs = [table[kr * p + t, k] for k in range(5)]
            block = -(-n // PIECES)
            for g in range(0, n, block):
                stencil_rows(xs, t % 2, coeffs, start + SUB * g, min(block, n - g))

    def take_late(side, p):
        @pl.when(p == 0)
        def _():
            take_columns(late, (early_rows, 0)[1 - side], late_rows)
            take_rows(side)

    def phase(p, _):
        @pl.when(part == 0)
        def _():
            take_halo(TOP, p)
            part_steps(p, True, -1)
            send_edge(TOP, p)
            take_late(BOTTOM, p)
            take_halo(BOTTOM, p)
            part_steps(p, False, -1)
            send_edge(BOTTOM, p)

        @pl.when(part == 1)
        def _():
            take_halo(BOTTOM, p)
            part_steps(p, True, 1)
            send_edge(BOTTOM, p)
            take_late(TOP, p)
            take_halo(TOP, p)
            part_steps(p, False, 1)
            send_edge(TOP, p)

        return 0

    lax.fori_loop(0, n_phase, phase, 0)

    inv = pow(NC, -1, LANES)
    idx = [(inv * (lane + (halo - c) % LANES)) & (LANES - 1) for c in range(NC)]

    wide = 4
    def to_natural(g, _):
        ats = [pl.multiple_of(SUB * (wide * g + k), SUB) for k in range(wide)]
        parts = {}
        for c in range(NC):
            for k in range(wide):
                for i in range(2):
                    parts[i, k, c] = permute(xs[i, c, pl.ds(base + ats[k], SUB), :], idx[c])
        for k in range(wide):
            for i, out in enumerate((nu, nv)):
                for b in range(nblk):
                    sel = [masks[(c - halo - LANES * b) % NC] for c in range(NC)]
                    out[pl.ds(kr + ats[k], SUB), b * LANES : (b + 1) * LANES] = pick(
                        sel, [parts[i, k, c] for c in range(NC)]
                    )
        return 0

    stores = []
    chunk = rows // 4
    for k in range(4):
        lax.fori_loop(k * chunk // (SUB * wide), (k + 1) * chunk // (SUB * wide), to_natural, 0, unroll=2)
        for i, (x, out) in enumerate(((nu, now_ref), (nv, old_ref))):
            stores.append(
                pltpu.make_async_copy(
                    x.at[pl.ds(kr + k * chunk, chunk)], out.at[pl.ds(k * chunk, chunk)], out_sem.at[i, k]
                )
            )
            stores[-1].start()
    for c in stores:
        c.wait()


def solution(mesh):
    row_n, col_n = mesh.shape["row"], mesh.shape["col"]
    spec = P(("ens", "row"), "col")

    def local_run(u, v, w):
        rows, cols = u.shape
        steps = w.shape[0]
        kr = 2 * SUB
        halo = (NC * LANES - cols) // 2
        tall = rows + 2 * kr
        f32 = jnp.float32
        out = jax.ShapeDtypeStruct(u.shape, f32)
        now, old = pl.pallas_call(
            functools.partial(kernel, rows, cols, steps, kr, halo, row_n, col_n),
            out_shape=(out, out),
            in_specs=[
                pl.BlockSpec(memory_space=pl.ANY),
                pl.BlockSpec(memory_space=pl.ANY),
                pl.BlockSpec(memory_space=pl.ANY),
            ],
            out_specs=(pl.BlockSpec(memory_space=pl.ANY), pl.BlockSpec(memory_space=pl.ANY)),
            scratch_shapes=[
                pltpu.SMEM((3, 3, steps), f32),
                pltpu.VMEM((steps, 5, SUB, LANES), f32),
                pltpu.VMEM((tall, cols), f32),
                pltpu.VMEM((tall, cols), f32),
                pltpu.VMEM((rows, LANES), f32),
                pltpu.VMEM((rows, LANES), f32),
                pltpu.VMEM((tall, LANES), f32),
                pltpu.VMEM((tall, LANES), f32),
                pltpu.VMEM((2, NC, rows + 2 * PAD, LANES), f32),
                pltpu.VMEM((2, 2, 2, NC, kr, LANES), f32),
                pltpu.SemaphoreType.REGULAR,
                pltpu.SemaphoreType.DMA((3,)),
                pltpu.SemaphoreType.DMA((2, 4)),
                pltpu.SemaphoreType.DMA((12,)),
                pltpu.SemaphoreType.DMA((12,)),
                pltpu.SemaphoreType.DMA((2, 2, 2)),
                pltpu.SemaphoreType.DMA((2, 2, 2)),
            ],
            compiler_params=pltpu.CompilerParams(collective_id=0, has_side_effects=True),
        )(u, v, jnp.transpose(w, (1, 2, 0)))
        return 4.0 * now, 8.0 * (now - old)

    return jax.shard_map(
        local_run, mesh=mesh, in_specs=(spec, spec, P()), out_specs=(spec, spec), check_vma=False
    )
```
